512 devices in a mesh: query: 4 (over x), cand: 32 (over z_hi, y, core), tensor: 4 (over z_lo).
Axes of the slice: x: 4, y: 4, z: 16 (z_hi: 4, z_lo: 4; z = z_hi * 4 + z_lo), core: 2. Of those that a mesh axis runs over, the one named last changes fastest.
Arguments:
- cand_states: bfloat16 [131072, 2048], P(('query', 'cand'), 'tensor'), parts along dimension 0, may hold values from -6 to 6
- prefix_states: bfloat16 [256, 2048], P(('query', 'cand'), 'tensor'), parts along dimension 0, may hold values from -6 to 6
- norm_gain: float32 [2048], replicated, may hold values from 0.5 to 1.5
- w_query: bfloat16 [2048, 1024], P(None, 'tensor'), may hold values from -1 to 1
- w_key: bfloat16 [2048, 256], P(None, 'tensor'), may hold values from -1 to 1
- w_value: bfloat16 [2048, 256], P(None, 'tensor'), may hold values from -0.125 to 0.125
- w_out: bfloat16 [1024, 2048], P('tensor'), may hold values from -1.5 to 1.5
- cand_lengths: int32 [1024], P(('query', 'cand')), parts along dimension 0, may hold values from 32 to 128, as said below
Outputs:
- attn_out: bfloat16 [131072, 2048], P(('query', 'cand', 'tensor')), parts along dimension 0
The draws below stay inside these ranges and needn't reach their ends.
There are 4 independent parts, one for each index of `query`. The reference program is written for one: setup_inputs(seed, part) draws one part's arguments, and reference() takes and returns one part's arrays. A program takes and returns all parts, laid end to end along the dimension named above; an argument that names none is the same for every part. Nothing has to cross between parts.
Inputs may be any that keep to these rules, and one draw needn't show every extreme that they name: `cand_lengths`: some candidate has all 128 slots live.
All inputs are finite; a program needn't handle non-finite values.
Results may differ from the reference program's by a relative error of at most 0.013.
Values may be sent and summed in bfloat16 or wider, within the bound.
A program may use at most 64 MiB of HBM per device.

```python
import jax
import jax.numpy as jnp
from jax import lax

D = 2048
HD = 256
PREFIX = 64
CLEN = 128
HEADS = 4
CANDS = 256
ROWS = 32768


def drawn_pair(key):
    shared = jax.random.normal(jax.random.fold_in(key, 11), (D, HD), jnp.float32) * D ** (-0.5)
    spread = jax.random.normal(jax.random.fold_in(key, 12), (D, HEADS * HD), jnp.float32) * D ** (-0.5)
    query_part = spread
    return (jnp.clip(query_part, -1.0, 1.0), jnp.clip(shared, -1.0, 1.0))


def draw_w_query(key, part):
    return drawn_pair(key)[0].astype(jnp.bfloat16)


def draw_w_key(key, part):
    return drawn_pair(key)[1].astype(jnp.bfloat16)


def draw_cand_lengths(key, part):
    lengths = jax.random.randint(jax.random.fold_in(key, 21), (CANDS,), CLEN // 4, CLEN + 1)
    chosen = jax.random.randint(jax.random.fold_in(key, 22), (), 0, CANDS)
    return lengths.at[chosen].set(CLEN).astype(jnp.int32)


def block_scale(stream_key, dims, pieces, low, high):
    def one(axis_at, parts):
        draws = jax.random.uniform(jax.random.fold_in(jax.random.fold_in(stream_key, 6), axis_at), (parts,), jnp.float32, low / len(pieces), high / len(pieces))
        return jnp.repeat(jnp.exp(draws), dims[axis_at] // parts).reshape((-1,) + (1,) * (len(dims) - axis_at - 1))

    loudness = one(*pieces[0])
    for cut in pieces[1:]:
        loudness = loudness * one(*cut)
    return loudness


def scatter_about(own_key, extent, deviation, reach, cuts=(), held_as=jnp.bfloat16):
    level = block_scale(own_key, extent, cuts, -0.22, 0.18) if cuts else 1.0
    values = jax.random.normal(own_key, extent, jnp.float32) * deviation * level
    return jnp.minimum(jnp.maximum(values, -reach), reach).astype(held_as)


def setup_inputs(seed: int = 0, part: int = 0) -> dict:
    arg_keys = jax.random.split(jax.random.key(seed), 9)
    part_keys = jax.random.split(jax.random.fold_in(arg_keys[8], part), 9)
    return {
        "cand_states": scatter_about(part_keys[0], (ROWS, D), 1.0, 6.0, ((0, 32), (1, 4))),
        "prefix_states": scatter_about(part_keys[1], (PREFIX, D), 1.0, 6.0, ((0, 32), (1, 4))),
        "norm_gain": jnp.clip(jax.random.uniform(arg_keys[2], (D,), jnp.float32, 0.5, 1.5), 0.5, 1.5),
        "w_query": draw_w_query(jax.random.fold_in(arg_keys[8], 71), part),
        "w_key": draw_w_key(jax.random.fold_in(arg_keys[8], 71), part),
        "w_value": scatter_about(arg_keys[5], (D, HD), D ** -0.5, 0.125, ((1, 4),)),
        "w_out": scatter_about(arg_keys[6], (HEADS * HD, D), 16 ** -0.5, 1.5, ((0, 4),)),
        "cand_lengths": draw_cand_lengths(jax.random.fold_in(jax.random.fold_in(arg_keys[8], part), 71), part),
    }


epsilon = 1e-06
theta_base = 10000.0

def rotate(values, positions):
    half_size = values.shape[-1] // 2
    frequency = theta_base ** (-jnp.arange(half_size, dtype=jnp.float32) * 2.0 / values.shape[-1])
    angles = positions.astype(jnp.float32)[:, None] * frequency[None, :]
    cosine = jnp.cos(angles)
    sine_part = jnp.sin(angles)
    lower_half = values[:, :half_size]
    upper_half = values[:, half_size:]
    return jnp.concatenate([lower_half * cosine - upper_half * sine_part, upper_half * cosine + lower_half * sine_part], axis=-1)

def normalize(states, norm_gain):
    values = states.astype(jnp.float32)
    square = lax.optimization_barrier(jnp.mean(values * values, axis=-1, keepdims=True))
    return (values * lax.rsqrt(square + epsilon) * norm_gain[None, :]).astype(jnp.bfloat16)

def rounded(values):
    return lax.optimization_barrier(values.astype(jnp.bfloat16)).astype(jnp.float32)

def reference(cand_states, prefix_states, norm_gain, w_query, w_key, w_value, w_out, cand_lengths):
    normed_cand = normalize(cand_states, norm_gain)
    normed_prefix = normalize(prefix_states, norm_gain)
    cand_pos = PREFIX + jnp.tile(jnp.arange(CLEN, dtype=jnp.int32), CANDS)
    prefix_pos = jnp.arange(PREFIX, dtype=jnp.int32)
    cand_keys = rotate(rounded(jnp.dot(normed_cand, w_key, preferred_element_type=jnp.float32)), cand_pos).astype(jnp.bfloat16)
    prefix_keys = rotate(rounded(jnp.dot(normed_prefix, w_key, preferred_element_type=jnp.float32)), prefix_pos).astype(jnp.bfloat16)
    cand_values = jnp.dot(normed_cand, w_value, preferred_element_type=jnp.float32).astype(jnp.bfloat16)
    prefix_values = jnp.dot(normed_prefix, w_value, preferred_element_type=jnp.float32).astype(jnp.bfloat16)
    key_blocks = cand_keys.astype(jnp.float32).reshape(CANDS, CLEN, HD)
    value_blocks = cand_values.astype(jnp.float32).reshape(CANDS, CLEN, HD)
    early_keys = prefix_keys.astype(jnp.float32)
    early_values = prefix_values.astype(jnp.float32)
    slots = jnp.arange(CLEN, dtype=jnp.int32)
    causal = slots[:, None] >= slots[None, :]
    live_rows = slots[None, :] < cand_lengths[:, None]
    summed_out = jnp.zeros((CANDS * CLEN, D), jnp.float32)
    for head_index in range(HEADS):
        query_cols = w_query[:, head_index * HD:(head_index + 1) * HD]
        query_rows = rotate(jnp.dot(normed_cand, query_cols, preferred_element_type=jnp.float32), cand_pos) * HD ** (-0.5)
        queries = rounded(query_rows).reshape(CANDS, CLEN, HD)
        self_scores = jnp.einsum('cqd,ckd->cqk', queries, key_blocks)
        self_scores = jnp.where(causal[None], self_scores, -jnp.inf)
        prefix_scores = jnp.einsum('cqd,kd->cqk', queries, early_keys)
        highest = jnp.maximum(self_scores.max(-1), prefix_scores.max(-1))[..., None]
        self_weights = jnp.exp(self_scores - highest)
        prefix_weights = jnp.exp(prefix_scores - highest)
        divisor = self_weights.sum(-1) + prefix_weights.sum(-1)
        mixture = jnp.einsum('cqk,ckd->cqd', rounded(self_weights), value_blocks)
        mixture = mixture + jnp.einsum('cqk,kd->cqd', rounded(prefix_weights), early_values)
        head_rows = jnp.where(live_rows[..., None], mixture / divisor[..., None], 0.0)
        head_rows = head_rows.reshape(CANDS * CLEN, HD).astype(jnp.bfloat16)
        head_term = jnp.dot(head_rows, w_out[head_index * HD:(head_index + 1) * HD], preferred_element_type=jnp.float32)
        summed_out = summed_out + rounded(head_term)
    return summed_out.astype(jnp.bfloat16)
```

```python
import numpy as np

import jax
import jax.numpy as jnp
from jax import lax
from jax.experimental import pallas as pl
from jax.experimental.pallas import tpu as pltpu
from jax.sharding import PartitionSpec as P

MESH = pl.DeviceIdType.MESH
BF16 = jnp.bfloat16
F32 = jnp.float32
EPS = 1e-06
THETA = 10000.0

NX = 4
NY = 4
NZ = 16
ZL = 4
CL = 128
HS = 256
D = 2048
FC = 512
PRE = 64


def rope_tables():
    half = HS // 2
    freq = (THETA ** (-np.arange(half, dtype=np.float32) * 2.0 / HS)).astype(np.float32)
    cand = (PRE + np.arange(CL)).astype(np.float32)
    core, y, zh, r = np.meshgrid(
        np.arange(2), np.arange(4), np.arange(4), np.arange(2), indexing="ij"
    )
    pre = ((zh * 8 + y * 2 + core) * 2 + r).reshape(-1).astype(np.float32)
    pos = np.concatenate([cand, pre])
    angles = (pos[:, None] * freq[None, :]).astype(np.float32).astype(np.float64)
    return np.cos(angles).astype(np.float32), np.sin(angles).astype(np.float32)


class Links:
    def __init__(self, ssem, rsem):
        self.ssem, self.rsem, self.made = ssem, rsem, []

    def send(self, src, dst, device):
        i = len(self.made)
        copy = pltpu.make_async_remote_copy(
            src_ref=src,
            dst_ref=dst,
            send_sem=self.ssem.at[i],
            recv_sem=self.rsem.at[i],
            device_id=device,
            device_id_type=MESH,
        )
        copy.start()
        self.made.append(copy)
        return copy

    def finish(self):
        for copy in self.made:
            copy.wait_send()


N_SEMS = 120


def kernel(
    states, prefix, gain, wq, wkv, wo, lens, cos_t, sin_t,
    out,
    A, B, xs, xb, pb, pf, xn, kvs, kc, vc, q4, hr, ob, ssem, rsem, lsem,
):
    x = lax.axis_index("query")
    cd = lax.axis_index("cand")
    t = lax.axis_index("tensor")
    zh = cd // 8
    y = (cd // 2) % 4
    c = cd % 2
    z = zh * 4 + t

    def at(xx, yy, zz, cc):
        return (xx, (zz // 4) * 8 + yy * 2 + cc, zz % 4)

    def m4(v):
        return (v + 8) % 4

    def zdev(dz):
        return at(x, y, (z + dz + 32) % 16, c)

    def tdev(k):
        return (x, cd, (t + k) % 4)

    xp, xm = at(m4(x + 1), y, z, c), at(m4(x - 1), y, z, c)
    yp, ym = at(x, m4(y + 1), z, c), at(x, m4(y - 1), z, c)
    yo = at(x, m4(y + 2), z, c)
    mate = at(x, y, z, 1 - c)

    def rows_a(xx, yy, off=0, n=64):
        return pl.ds(pl.multiple_of(64 * (c * 16 + yy * 4 + xx) + off, 32), n)

    def cols_b(xx, yy):
        return pl.ds(pl.multiple_of(128 * (xx * 4 + yy), 128), 128)

    def rows_b(off=0, n=128):
        return pl.ds(pl.multiple_of(128 * c + off, 64), n)

    def slice_a(xx, yy, off=0, n=64):
        return A.at[1:4, rows_a(xx, yy, off, n), :]

    def slice_b(xx, yy, off=0, n=128):
        return B.at[1:4, rows_b(off, n), cols_b(xx, yy)]

    def local(i, src, dst):
        copy = pltpu.make_async_copy(src, dst, lsem.at[i])
        copy.start()
        return copy

    lp = local(0, prefix, pb.at[c, y, z])
    lq = local(1, wq, A.at[0, :, 0:256])
    lkv = local(2, wkv, A.at[0, :, 256:384])
    lo = local(3, wo, B.at[0])
    ls = local(4, states, xs)
    lx = local(5, states.at[pl.ds(pl.multiple_of(256 * t, 256), 256), :], xb.at[t])

    barrier = pltpu.get_barrier_semaphore()
    near = [zdev(d) for d in (-4, -3, -2, -1, 1, 2, 3, 4)]
    near += [xp, xm, yp, ym, yo, mate]
    for device in near:
        pl.semaphore_signal(barrier, inc=1, device_id=device, device_id_type=MESH)
    pl.semaphore_wait(barrier, len(near))

    net = Links(ssem, rsem)

    lp.wait()
    tile = pb.at[c, y, z]
    pz = {d: net.send(tile, tile, zdev(d)) for d in (4, -4, 1, -1, 2, -2, 3, -3)}

    lq.wait()
    lkv.wait()
    pa = []
    for k in (2, 1, 3):
        src = A.at[0, rows_a(x, y), :]
        pa.append(net.send(src, A.at[4 - k, rows_a(x, y), :], tdev(k)))
    lo.wait()
    pbq = []
    for k in (2, 1, 3):
        src = B.at[0, rows_b(), cols_b(x, y)]
        pbq.append(net.send(src, B.at[4 - k, rows_b(), cols_b(x, y)], tdev(k)))

    pz[4].wait_recv()
    pz[-4].wait_recv()
    low = pb.at[c, y, (z + 12) % 16]
    high = pb.at[c, y, (z + 4) % 16]
    pz2 = [net.send(low, low, zdev(d)) for d in (4, 3, 2, 1)]
    pz2 += [net.send(high, high, zdev(d)) for d in (-3, -2, -1)]

    ls.wait()
    st = []
    for cc in range(2):
        part = []
        for k in (2, 1, 3):
            peer = (t + k) % 4
            src = xs.at[pl.ds(pl.multiple_of(256 * peer + 128 * cc, 128), 128), :]
            dst = xb.at[t, pl.ds(128 * cc, 128), :]
            part.append(net.send(src, dst, tdev(k)))
        st.append(part)

    for copy in pa:
        copy.wait_recv()
    own_a, own_b = slice_a(x, y), slice_b(x, y)
    a_xp = net.send(own_a, own_a, xp)
    a_xm = net.send(own_a, own_a, xm)
    for copy in pbq:
        copy.wait_recv()
    b_yp = net.send(own_b, own_b, yp)
    b_ym = net.send(own_b, own_b, ym)
    ya = {0: (net.send(own_a, own_a, yp), net.send(own_a, own_a, ym))}
    xbp = {0: (net.send(own_b, own_b, xp), net.send(own_b, own_b, xm))}

    for d in (-3, -2, -1, 1, 2, 3):
        pz[d].wait_recv()
    for copy in pz2:
        copy.wait_recv()
    line = pb.at[c, y]
    py = [net.send(line, line, d) for d in (yp, ym, yo)]

    def slice_fwd(first, second):
        pass

    a_xp.wait_recv()
    h = slice_a(m4(x - 1), y, 0, 32)
    a_xp2 = net.send(h, h, xp)
    s = slice_a(m4(x - 1), y)
    ya[-1] = (net.send(s, s, yp), net.send(s, s, ym))
    b_yp.wait_recv()
    h = slice_b(x, m4(y - 1), 0, 64)
    b_yp2 = net.send(h, h, yp)
    s = slice_b(x, m4(y - 1))
    xbp[-1] = (net.send(s, s, xp), net.send(s, s, xm))
    a_xm.wait_recv()
    h = slice_a(m4(x + 1), y, 32, 32)
    a_xm2 = net.send(h, h, xm)
    s = slice_a(m4(x + 1), y)
    ya[1] = (net.send(s, s, yp), net.send(s, s, ym))
    b_ym.wait_recv()
    h = slice_b(x, m4(y + 1), 64, 64)
    b_ym2 = net.send(h, h, ym)
    s = slice_b(x, m4(y + 1))
    xbp[1] = (net.send(s, s, xp), net.send(s, s, xm))

    for copy in py:
        copy.wait_recv()
    pm = net.send(pb.at[c], pb.at[c], mate)

    a_xp2.wait_recv()
    a_xm2.wait_recv()
    s = slice_a(m4(x + 2), y)
    ya[2] = (net.send(s, s, yp), net.send(s, s, ym))
    b_yp2.wait_recv()
    b_ym2.wait_recv()
    s = slice_b(x, m4(y + 2))
    xbp[2] = (net.send(s, s, xp), net.send(s, s, xm))

    def set_a(yy):
        return A.at[1:4, pl.ds(pl.multiple_of(64 * (c * 16 + yy * 4), 256), 256), :]

    def set_b(xx):
        return B.at[1:4, rows_b(), pl.ds(pl.multiple_of(512 * xx, 512), 512)]

    mates = [net.send(set_a(y), set_a(y), mate), net.send(set_b(x), set_b(x), mate)]

    fwd = []
    for dx in (0, -1, 1, 2):
        ya[dx][0].wait_recv()
        h = slice_a(m4(x + dx), m4(y - 1), 0, 32)
        fwd.append(net.send(h, h, yp))
        xbp[dx][0].wait_recv()
        h = slice_b(m4(x - 1), m4(y + dx), 0, 64)
        fwd.append(net.send(h, h, xp))
        ya[dx][1].wait_recv()
        h = slice_a(m4(x + dx), m4(y + 1), 32, 32)
        fwd.append(net.send(h, h, ym))
        xbp[dx][1].wait_recv()
        h = slice_b(m4(x + 1), m4(y + dx), 64, 64)
        fwd.append(net.send(h, h, xm))
    for s in (set_a(m4(y - 1)), set_b(m4(x - 1)), set_a(m4(y + 1)), set_b(m4(x + 1))):
        mates.append(net.send(s, s, mate))

    lx.wait()

    def norm_cand(cc):
        rows = pl.ds(128 * cc, 128)
        total = jnp.zeros((128, 1), F32)
        for f in range(4):
            v = xb[f, rows, :].astype(F32)
            total += jnp.sum(v * v, axis=-1, keepdims=True)
        scale = lax.rsqrt(total * (1.0 / D) + EPS)
        for f in range(4):
            v = xb[f, rows, :].astype(F32)
            g = gain[:, FC * f : FC * (f + 1)]
            xn[rows, FC * f : FC * (f + 1)] = (v * scale * g).astype(BF16)

    for copy in st[0]:
        copy.wait_recv()
    norm_cand(0)

    pm.wait_recv()
    for f in range(4):
        for cc in range(2):
            for yy in range(4):
                for hh in range(4):
                    at_row = ((cc * 4 + yy) * 4 + hh) * 8
                    pf[f, at_row : at_row + 8, :] = pb[cc, yy, hh * 4 + f].astype(F32)
    pieces = [
        [pf[f, pl.ds(k, PRE, stride=4), :] for k in range(4)] for f in range(4)
    ]
    total = jnp.zeros((PRE, 1), F32)
    for row in pieces:
        for v in row:
            total += jnp.sum(v * v, axis=-1, keepdims=True)
    scale = lax.rsqrt(total * (1.0 / D) + EPS)
    for f in range(4):
        for k in range(4):
            lo_col = FC * f + 128 * k
            g = gain[:, lo_col : lo_col + 128]
            xn[256:320, lo_col : lo_col + 128] = (pieces[f][k] * scale * g).astype(BF16)

    for copy in fwd:
        copy.wait_recv()
    for s in (set_a(m4(y + 2)), set_b(m4(x + 2))):
        mates.append(net.send(s, s, mate))
    for copy in mates:
        copy.wait_recv()

    def rotate(v, cos, sin):
        a, b = v[:, :128], v[:, 128:]
        return jnp.concatenate([a * cos - b * sin, b * cos + a * sin], axis=-1)

    def project_kv(rows, n, table, key_rows, cc):
        xv = xn[rows, :]
        for pair in range(2):
            w = jnp.concatenate([A[2 * pair, :, 256:384], A[2 * pair + 1, :, 256:384]], axis=-1)
            r = jnp.dot(xv, w, preferred_element_type=F32)
            kvs[2 * pair, 0:n, :] = r[:, :128]
            kvs[2 * pair + 1, 0:n, :] = r[:, 128:]
        parts = [kvs[(f - t + 4) % 4, 0:n, :] for f in range(4)]
        key = jnp.concatenate([p[:, :64] for p in parts], axis=-1)
        val = jnp.concatenate([p[:, 64:] for p in parts], axis=-1)
        kc[key_rows, :] = rotate(key, cos_t[table, :], sin_t[table, :]).astype(BF16)
        vc[key_rows, :] = val.astype(BF16)

    project_kv(pl.ds(256, PRE), PRE, pl.ds(CL, PRE), pl.ds(CL, PRE), None)

    outs = []
    for cc in range(2):
        rows = pl.ds(128 * cc, 128)
        if cc == 1:
            for copy in st[1]:
                copy.wait_recv()
            norm_cand(1)
        project_kv(rows, CL, pl.ds(0, CL), pl.ds(0, CL), cc)

        def head(r, carry, rows=rows):
            qv = jnp.dot(xn[rows, :], A[r, :, 0:256], preferred_element_type=F32)
            qv = rotate(qv, cos_t[0:CL, :], sin_t[0:CL, :]) * (HS ** -0.5)
            q4[pl.ds(pl.multiple_of(r * CL, CL), CL), :] = qv.astype(BF16)
            return carry

        lax.fori_loop(0, 4, head, 0)
        live = lens[2 * t + cc]

        scores = lax.dot_general(
            q4[...], kc[...], (((1,), (1,)), ((), ())), preferred_element_type=F32
        )
        row = lax.broadcasted_iota(jnp.int32, scores.shape, 0) % CL
        col = lax.broadcasted_iota(jnp.int32, scores.shape, 1)
        scores = jnp.where((col <= row) | (col >= CL), scores, -jnp.inf)
        weights = jnp.exp(scores - jnp.max(scores, axis=-1, keepdims=True))
        divisor = jnp.sum(weights, axis=-1, keepdims=True)
        mix = jnp.dot(weights.astype(BF16), vc[...], preferred_element_type=F32) / divisor
        slot = lax.broadcasted_iota(jnp.int32, mix.shape, 0) % CL
        hr[...] = jnp.where(slot < live, mix, 0.0).astype(BF16)

        def out_cols(n, carry, rows=rows):
            cols = pl.ds(pl.multiple_of(n * 512, 512), 512)
            acc = jnp.zeros((CL, 512), F32)
            for r in range(4):
                acc += jnp.dot(
                    hr[r * CL : (r + 1) * CL, :], B[r, :, cols], preferred_element_type=F32
                )
            ob[rows, cols] = acc.astype(BF16)
            return carry

        lax.fori_loop(0, 4, out_cols, 0)
        outs.append(local(6 + cc, ob.at[rows, :], out.at[rows, :]))

    net.finish()
    for copy in outs:
        copy.wait()


def body(cand_states, prefix_states, norm_gain, w_query, w_key, w_value, w_out, cand_lengths):
    cos_np, sin_np = rope_tables()
    prefix = prefix_states.reshape(8, 128)
    wkv = jnp.concatenate([w_key, w_value], axis=1)
    any_spec = pl.BlockSpec(memory_space=pl.ANY)
    vmem = pl.BlockSpec(memory_space=pltpu.VMEM)
    smem = pl.BlockSpec(memory_space=pltpu.SMEM)
    return pl.pallas_call(
        kernel,
        out_shape=jax.ShapeDtypeStruct((256, D), BF16),
        in_specs=[any_spec, any_spec, vmem, any_spec, any_spec, any_spec, smem, vmem, vmem],
        out_specs=any_spec,
        scratch_shapes=[
            pltpu.VMEM((4, D, 384), BF16),
            pltpu.VMEM((4, HS, D), BF16),
            pltpu.VMEM((1024, FC), BF16),
            pltpu.VMEM((4, 256, FC), BF16),
            pltpu.VMEM((2, 4, 16, 8, 128), BF16),
            pltpu.VMEM((4, 256, 128), F32),
            pltpu.VMEM((320, D), BF16),
            pltpu.VMEM((4, CL, 128), F32),
            pltpu.VMEM((CL + PRE, HS), BF16),
            pltpu.VMEM((CL + PRE, HS), BF16),
            pltpu.VMEM((4 * CL, HS), BF16),
            pltpu.VMEM((4 * CL, HS), BF16),
            pltpu.VMEM((256, D), BF16),
            pltpu.SemaphoreType.DMA((N_SEMS,)),
            pltpu.SemaphoreType.DMA((N_SEMS,)),
            pltpu.SemaphoreType.DMA((8,)),
        ],
        compiler_params=pltpu.CompilerParams(
            collective_id=0, has_side_effects=True, vmem_limit_bytes=56 * 1024 * 1024
        ),
        name="sublayer",
    )(
        cand_states, prefix, norm_gain.reshape(1, D), w_query, wkv, w_out, cand_lengths,
        jnp.asarray(cos_np), jnp.asarray(sin_np),
    )


def solution(mesh):
    in_specs = (
        P(("query", "cand"), "tensor"),
        P(("query", "cand"), "tensor"),
        P(),
        P(None, "tensor"),
        P(None, "tensor"),
        P(None, "tensor"),
        P("tensor", None),
        P(("query", "cand")),
    )
    out_specs = P(("query", "cand", "tensor"), None)
    return jax.shard_map(body, mesh=mesh, in_specs=in_specs, out_specs=out_specs, check_vma=False)
```

```python
import numpy as np

import jax
import jax.numpy as jnp
from jax import lax
from jax.experimental import pallas as pl
from jax.experimental.pallas import tpu as pltpu
from jax.sharding import PartitionSpec as P

MESH = pl.DeviceIdType.MESH
BF16 = jnp.bfloat16
F32 = jnp.float32
EPS = 1e-06
THETA = 10000.0

NX = 4
NY = 4
NZ = 16
ZL = 4
CL = 128
HS = 256
D = 2048
FC = 512
PRE = 64


def rope_tables():
    half = HS // 2
    freq = (THETA ** (-np.arange(half, dtype=np.float32) * 2.0 / HS)).astype(np.float32)
    cand = (PRE + np.arange(CL)).astype(np.float32)
    core, y, zh, r = np.meshgrid(
        np.arange(2), np.arange(4), np.arange(4), np.arange(2), indexing="ij"
    )
    pre = ((zh * 8 + y * 2 + core) * 2 + r).reshape(-1).astype(np.float32)
    pos = np.concatenate([pre, cand])
    angles = (pos[:, None] * freq[None, :]).astype(np.float32).astype(np.float64)
    return np.cos(angles).astype(np.float32), np.sin(angles).astype(np.float32)


class Links:
    def __init__(self, ssem, rsem):
        self.ssem, self.rsem, self.made = ssem, rsem, []

    def send(self, src, dst, device):
        i = len(self.made)
        copy = pltpu.make_async_remote_copy(
            src_ref=src,
            dst_ref=dst,
            send_sem=self.ssem.at[i],
            recv_sem=self.rsem.at[i],
            device_id=device,
            device_id_type=MESH,
        )
        copy.start()
        self.made.append(copy)
        return copy

    def finish(self):
        for copy in self.made:
            copy.wait_send()


N_SEMS = 128
NPRE = PRE


def kernel(
    states, prefix, gain_h, wq, wk, wv, wo, lens_h, cos_h, sin_h,
    out,
    A, B, xs, xb, pb, pf, xn, kvs, kc, vc, q4, hr, ob, gain, cos_t, sin_t, lens,
    ssem, rsem, lsem,
):
    x = lax.axis_index("query")
    cd = lax.axis_index("cand")
    t = lax.axis_index("tensor")
    zh = cd // 8
    y = (cd // 2) % 4
    c = cd % 2
    z = zh * 4 + t

    def at(xx, yy, zz, cc):
        return (xx, (zz // 4) * 8 + yy * 2 + cc, zz % 4)

    def m4(v):
        return (v + 8) % 4

    def zdev(dz):
        return at(x, y, (z + dz + 32) % 16, c)

    def tdev(k):
        return (x, cd, (t + k) % 4)

    xp, xm = at(m4(x + 1), y, z, c), at(m4(x - 1), y, z, c)
    yp, ym = at(x, m4(y + 1), z, c), at(x, m4(y - 1), z, c)
    yo = at(x, m4(y + 2), z, c)
    mate = at(x, y, z, 1 - c)

    def rows_a(xx, yy, off=0, n=64):
        return pl.ds(pl.multiple_of(64 * (c * 16 + yy * 4 + xx) + off, 32), n)

    def cols_b(xx, yy):
        return pl.ds(pl.multiple_of(128 * (xx * 4 + yy), 128), 128)

    def rows_b(off=0, n=192):
        return pl.ds(pl.multiple_of(192 * c + off, 96), n)

    def slice_a(xx, yy, off=0, n=64):
        return A.at[1:4, rows_a(xx, yy, off, n), :]

    def slice_b(xx, yy, off=0, n=192):
        return B.at[1:4, rows_b(off, n), cols_b(xx, yy)]

    def local(i, src, dst):
        copy = pltpu.make_async_copy(src, dst, lsem.at[i])
        copy.start()
        return copy

    lp = local(0, prefix, pb.at[c, y, z])
    lq = local(1, wq, A.at[0])
    lo = [
        local(2, wk, B.at[0, 256:320, :]),
        local(3, wv, B.at[0, 320:384, :]),
        local(4, wo, B.at[0, 0:256, :]),
    ]
    ls = local(5, states, xs)
    lx = local(6, states.at[pl.ds(pl.multiple_of(256 * t, 256), 256), :], xb.at[t])
    small = [
        local(7, gain_h, gain),
        local(8, cos_h, cos_t),
        local(9, sin_h, sin_t),
        local(10, lens_h, lens),
    ]

    net = Links(ssem, rsem)

    lq.wait()
    pa = []
    for k in (2, 1, 3):
        src = A.at[0, rows_a(x, y), :]
        pa.append(net.send(src, A.at[4 - k, rows_a(x, y), :], tdev(k)))
    for copy in lo:
        copy.wait()
    pbq = []
    for k in (2, 1, 3):
        src = B.at[0, rows_b(), cols_b(x, y)]
        pbq.append(net.send(src, B.at[4 - k, rows_b(), cols_b(x, y)], tdev(k)))

    lp.wait()
    tile = pb.at[c, y, z]
    pz = [net.send(tile, tile, zdev(d)) for d in (8, 7, -7, 6, -6, 5, -5, 4, -4, 3, -3, 2, -2, 1, -1)]

    ls.wait()
    st = []
    for cc in range(2):
        part = []
        for k in (2, 1, 3):
            peer = (t + k) % 4
            src = xs.at[pl.ds(pl.multiple_of(256 * peer + 128 * cc, 128), 128), :]
            dst = xb.at[t, pl.ds(128 * cc, 128), :]
            part.append(net.send(src, dst, tdev(k)))
        st.append(part)

    for copy in pa:
        copy.wait_recv()
    own_a, own_b = slice_a(x, y), slice_b(x, y)
    a_xp = net.send(own_a, own_a, xp)
    a_xm = net.send(own_a, own_a, xm)
    for copy in pbq:
        copy.wait_recv()
    b_yp = net.send(own_b, own_b, yp)
    b_ym = net.send(own_b, own_b, ym)
    ya = {0: (net.send(own_a, own_a, yp), net.send(own_a, own_a, ym))}
    xbp = {0: (net.send(own_b, own_b, xp), net.send(own_b, own_b, xm))}

    a_xp.wait_recv()
    h = slice_a(m4(x - 1), y, 0, 32)
    a_xp2 = net.send(h, h, xp)
    s = slice_a(m4(x - 1), y)
    ya[-1] = (net.send(s, s, yp), net.send(s, s, ym))
    a_xm.wait_recv()
    h = slice_a(m4(x + 1), y, 32, 32)
    a_xm2 = net.send(h, h, xm)
    s = slice_a(m4(x + 1), y)
    ya[1] = (net.send(s, s, yp), net.send(s, s, ym))
    b_yp.wait_recv()
    h = slice_b(x, m4(y - 1), 0, 96)
    b_yp2 = net.send(h, h, yp)
    s = slice_b(x, m4(y - 1))
    xbp[-1] = (net.send(s, s, xp), net.send(s, s, xm))
    b_ym.wait_recv()
    h = slice_b(x, m4(y + 1), 96, 96)
    b_ym2 = net.send(h, h, ym)
    s = slice_b(x, m4(y + 1))
    xbp[1] = (net.send(s, s, xp), net.send(s, s, xm))

    a_xp2.wait_recv()
    a_xm2.wait_recv()
    s = slice_a(m4(x + 2), y)
    ya[2] = (net.send(s, s, yp), net.send(s, s, ym))
    b_yp2.wait_recv()
    b_ym2.wait_recv()
    s = slice_b(x, m4(y + 2))
    xbp[2] = (net.send(s, s, xp), net.send(s, s, xm))

    def set_a(yy):
        return A.at[1:4, pl.ds(pl.multiple_of(64 * (c * 16 + yy * 4), 256), 256), :]

    def set_b(xx):
        return B.at[1:4, rows_b(), pl.ds(pl.multiple_of(512 * xx, 512), 512)]

    mates = [net.send(set_a(y), set_a(y), mate), net.send(set_b(x), set_b(x), mate)]

    fwd = {}
    for dx in (0, -1, 1, 2):
        ya[dx][0].wait_recv()
        h = slice_a(m4(x + dx), m4(y - 1), 0, 32)
        f0 = net.send(h, h, yp)
        ya[dx][1].wait_recv()
        h = slice_a(m4(x + dx), m4(y + 1), 32, 32)
        f1 = net.send(h, h, ym)
        xbp[dx][0].wait_recv()
        h = slice_b(m4(x - 1), m4(y + dx), 0, 96)
        f2 = net.send(h, h, xp)
        xbp[dx][1].wait_recv()
        h = slice_b(m4(x + 1), m4(y + dx), 96, 96)
        f3 = net.send(h, h, xm)
        fwd[dx] = (f0, f1, f2, f3)
        if dx == -1:
            for copy in pz:
                copy.wait_recv()
            line = pb.at[c, y]
            py = [net.send(line, line, d) for d in (yo, yp, ym)]
    for s in (set_a(m4(y - 1)), set_a(m4(y + 1)), set_b(m4(x - 1)), set_b(m4(x + 1))):
        mates.append(net.send(s, s, mate))
    for copy in py:
        copy.wait_recv()
    pm = net.send(pb.at[c], pb.at[c], mate)

    lx.wait()
    for copy in small:
        copy.wait()

    def norm_cand(cc):
        rows = pl.ds(128 * cc, 128)
        into = pl.ds(NPRE + 128 * cc, 128)
        total = jnp.zeros((128, 1), F32)
        for f in range(4):
            v = xb[f, rows, :].astype(F32)
            total += jnp.sum(v * v, axis=-1, keepdims=True)
        scale = lax.rsqrt(total * (1.0 / D) + EPS)
        for f in range(4):
            v = xb[f, rows, :].astype(F32)
            g = gain[:, FC * f : FC * (f + 1)]
            xn[into, FC * f : FC * (f + 1)] = (v * scale * g).astype(BF16)

    for copy in st[0]:
        copy.wait_recv()
    norm_cand(0)

    for dx in (0, -1, 1, 2):
        f0, f1, f2, f3 = fwd[dx]
        f0.wait_recv()
        f1.wait_recv()
        s = slice_a(m4(x + dx), m4(y + 2))
        mates.append(net.send(s, s, mate))
        f2.wait_recv()
        f3.wait_recv()
        s = slice_b(m4(x + 2), m4(y + dx))
        mates.append(net.send(s, s, mate))

    pm.wait_recv()
    for f in range(4):
        for g in range(32):
            pf[f, 2 * g : 2 * g + 2, :] = pb[g // 16, (g // 4) % 4, (g % 4) * 4 + f].astype(F32)
    total = jnp.zeros((PRE, 1), F32)
    for f in range(4):
        total += jnp.sum(pf[f] * pf[f], axis=-1, keepdims=True)
    scale = lax.rsqrt(total * (1.0 / D) + EPS)
    for f in range(4):
        g = gain[:, FC * f : FC * (f + 1)]
        xn[0:PRE, FC * f : FC * (f + 1)] = (pf[f] * scale * g).astype(BF16)

    for copy in mates:
        copy.wait_recv()

    def rotate(v, cos, sin):
        a, b = v[:, :128], v[:, 128:]
        return jnp.concatenate([a * cos - b * sin, b * cos + a * sin], axis=-1)

    def project_kv(start, n, first):
        xv = xn[start : start + n, :]
        for pair in range(2):
            w = jnp.concatenate([B[2 * pair, 256:384, :], B[2 * pair + 1, 256:384, :]], axis=0)
            r = lax.dot_general(xv, w, (((1,), (1,)), ((), ())), preferred_element_type=F32)
            kvs[2 * pair, 0:n, :] = r[:, :128]
            kvs[2 * pair + 1, 0:n, :] = r[:, 128:]
        parts = [kvs[(f - t + 4) % 4, 0:n, :] for f in range(4)]
        key = jnp.concatenate([p[:, :64] for p in parts], axis=-1)
        val = jnp.concatenate([p[:, 64:] for p in parts], axis=-1)
        into = pl.ds(first, n)
        kc[into, :] = rotate(key, cos_t[into, :], sin_t[into, :]).astype(BF16)
        vc[into, :] = val.astype(BF16)

    outs = []
    for cc in range(2):
        rows = pl.ds(128 * cc, 128)
        xrows = pl.ds(NPRE + 128 * cc, 128)
        if cc == 0:
            project_kv(0, PRE + CL, 0)
        else:
            for copy in st[1]:
                copy.wait_recv()
            norm_cand(1)
            project_kv(PRE + CL, CL, PRE)

        def head(r, carry, xrows=xrows):
            qv = jnp.dot(xn[xrows, :], A[r], preferred_element_type=F32)
            qv = rotate(qv, cos_t[PRE:, :], sin_t[PRE:, :]) * (HS ** -0.5)
            q4[pl.ds(pl.multiple_of(r * CL, CL), CL), :] = qv.astype(BF16)
            return carry

        lax.fori_loop(0, 4, head, 0)
        live = lens[2 * t + cc]

        scores = lax.dot_general(
            q4[...], kc[...], (((1,), (1,)), ((), ())), preferred_element_type=F32
        )
        row = lax.broadcasted_iota(jnp.int32, scores.shape, 0) % CL
        col = lax.broadcasted_iota(jnp.int32, scores.shape, 1)
        scores = jnp.where(col <= row + PRE, scores, -jnp.inf)
        weights = jnp.exp(scores - jnp.max(scores, axis=-1, keepdims=True))
        divisor = jnp.sum(weights, axis=-1, keepdims=True)
        mix = jnp.dot(weights.astype(BF16), vc[...], preferred_element_type=F32) / divisor
        slot = lax.broadcasted_iota(jnp.int32, mix.shape, 0) % CL
        hr[...] = jnp.where(slot < live, mix, 0.0).astype(BF16)

        def out_cols(n, carry, rows=rows):
            cols = pl.ds(pl.multiple_of(n * 512, 512), 512)
            acc = jnp.zeros((CL, 512), F32)
            for r in range(4):
                acc += jnp.dot(
                    hr[r * CL : (r + 1) * CL, :], B[r, 0:256, cols], preferred_element_type=F32
                )
            ob[rows, cols] = acc.astype(BF16)
            return carry

        lax.fori_loop(0, 4, out_cols, 0)
        outs.append(local(11 + cc, ob.at[rows, :], out.at[rows, :]))

    net.finish()
    for copy in outs:
        copy.wait()


def body(cand_states, prefix_states, norm_gain, w_query, w_key, w_value, w_out, cand_lengths):
    cos_np, sin_np = rope_tables()
    any_spec = pl.BlockSpec(memory_space=pl.ANY)
    return pl.pallas_call(
        kernel,
        out_shape=jax.ShapeDtypeStruct((256, D), BF16),
        in_specs=[any_spec] * 10,
        out_specs=any_spec,
        scratch_shapes=[
            pltpu.VMEM((4, D, HS), BF16),
            pltpu.VMEM((4, 384, D), BF16),
            pltpu.VMEM((1024, FC), BF16),
            pltpu.VMEM((4, 256, FC), BF16),
            pltpu.VMEM((2, 4, 16, 2, FC), BF16),
            pltpu.VMEM((4, PRE, FC), F32),
            pltpu.VMEM((320, D), BF16),
            pltpu.VMEM((4, PRE + CL, 128), F32),
            pltpu.VMEM((CL + PRE, HS), BF16),
            pltpu.VMEM((CL + PRE, HS), BF16),
            pltpu.VMEM((4 * CL, HS), BF16),
            pltpu.VMEM((4 * CL, HS), BF16),
            pltpu.VMEM((256, D), BF16),
            pltpu.VMEM((1, D), F32),
            pltpu.VMEM((PRE + CL, 128), F32),
            pltpu.VMEM((PRE + CL, 128), F32),
            pltpu.SMEM((8,), jnp.int32),
            pltpu.SemaphoreType.DMA((N_SEMS,)),
            pltpu.SemaphoreType.DMA((N_SEMS,)),
            pltpu.SemaphoreType.DMA((16,)),
        ],
        compiler_params=pltpu.CompilerParams(
            has_side_effects=True, vmem_limit_bytes=56 * 1024 * 1024
        ),
        name="sublayer",
    )(
        cand_states, prefix_states, norm_gain.reshape(1, D), w_query, w_key.T, w_value.T,
        w_out, cand_lengths, jnp.asarray(cos_np), jnp.asarray(sin_np),
    )


def solution(mesh):
    in_specs = (
        P(("query", "cand"), "tensor"),
        P(("query", "cand"), "tensor"),
        P(),
        P(None, "tensor"),
        P(None, "tensor"),
        P(None, "tensor"),
        P("tensor", None),
        P(("query", "cand")),
    )
    out_specs = P(("query", "cand", "tensor"), None)
    return jax.shard_map(body, mesh=mesh, in_specs=in_specs, out_specs=out_specs, check_vma=False)
```

```python
import numpy as np

import jax
import jax.numpy as jnp
from jax import lax
from jax.experimental import pallas as pl
from jax.experimental.pallas import tpu as pltpu
from jax.sharding import PartitionSpec as P

MESH = pl.DeviceIdType.MESH
BF16 = jnp.bfloat16
F32 = jnp.float32
EPS = 1e-06
THETA = 10000.0

NX = 4
NY = 4
NZ = 16
ZL = 4
CL = 128
HS = 256
D = 2048
FC = 512
PRE = 64


def rope_tables():
    half = HS // 2
    freq = (THETA ** (-np.arange(half, dtype=np.float32) * 2.0 / HS)).astype(np.float32)
    cand = (PRE + np.arange(CL)).astype(np.float32)
    core, y, zh, r = np.meshgrid(
        np.arange(2), np.arange(4), np.arange(4), np.arange(2), indexing="ij"
    )
    pre = ((zh * 8 + y * 2 + core) * 2 + r).reshape(-1).astype(np.float32)
    pos = np.concatenate([pre, cand])
    angles = (pos[:, None] * freq[None, :]).astype(np.float32).astype(np.float64)
    return np.cos(angles).astype(np.float32), np.sin(angles).astype(np.float32)


class Links:
    def __init__(self, ssem, rsem):
        self.ssem, self.rsem, self.made = ssem, rsem, []

    def send(self, src, dst, device):
        i = len(self.made)
        copy = pltpu.make_async_remote_copy(
            src_ref=src,
            dst_ref=dst,
            send_sem=self.ssem.at[i],
            recv_sem=self.rsem.at[i],
            device_id=device,
            device_id_type=MESH,
        )
        copy.start()
        self.made.append(copy)
        return copy

    def finish(self):
        for copy in self.made:
            copy.wait_send()


N_SEMS = 128
NPRE = PRE


def kernel(
    states, prefix, gain_h, wq, wk, wv, wo, lens_h, cos_h, sin_h,
    out,
    A, B, xs, xb, pb, pf, xn, kvs, kc, vc, q4, hr, ob, gain, cos_t, sin_t, lens,
    ssem, rsem, lsem, psem, qsem, go,
):
    x = lax.axis_index("query")
    cd = lax.axis_index("cand")
    t = lax.axis_index("tensor")
    zh = cd // 8
    y = (cd // 2) % 4
    c = cd % 2
    z = zh * 4 + t

    def at(xx, yy, zz, cc):
        return (xx, (zz // 4) * 8 + yy * 2 + cc, zz % 4)

    def m4(v):
        return (v + 8) % 4

    def zdev(dz):
        return at(x, y, (z + dz + 32) % 16, c)

    def tdev(k):
        return (x, cd, (t + k) % 4)

    xp, xm = at(m4(x + 1), y, z, c), at(m4(x - 1), y, z, c)
    yp, ym = at(x, m4(y + 1), z, c), at(x, m4(y - 1), z, c)
    yo = at(x, m4(y + 2), z, c)
    mate = at(x, y, z, 1 - c)

    def rows_a(xx, yy, off=0, n=64):
        return pl.ds(pl.multiple_of(64 * (c * 16 + yy * 4 + xx) + off, 32), n)

    def cols_b(xx, yy):
        return pl.ds(pl.multiple_of(128 * (xx * 4 + yy), 128), 128)

    def rows_b(off=0, n=192):
        return pl.ds(pl.multiple_of(192 * c + off, 96), n)

    def slice_a(xx, yy, off=0, n=64):
        return A.at[1:4, rows_a(xx, yy, off, n), :]

    def slice_b(xx, yy, off=0, n=192):
        return B.at[1:4, rows_b(off, n), cols_b(xx, yy)]

    def local(i, src, dst):
        copy = pltpu.make_async_copy(src, dst, lsem.at[i])
        copy.start()
        return copy

    lp = local(0, prefix, pb.at[c, y, z])
    lq = local(1, wq, A.at[0])
    lo = [
        local(2, wk, B.at[0, 256:320, :]),
        local(3, wv, B.at[0, 320:384, :]),
        local(4, wo, B.at[0, 0:256, :]),
    ]
    ls = local(5, states, xs)
    lx = local(6, states.at[pl.ds(pl.multiple_of(256 * t, 256), 256), :], xb.at[t])
    small = [
        local(7, gain_h, gain),
        local(8, cos_h, cos_t),
        local(9, sin_h, sin_t),
        local(10, lens_h, lens),
    ]

    up_edge = (t == 3) & (zh < 3)
    down_edge = (t == 0) & (zh > 0)
    up1, down1 = zdev(1), zdev(-1)
    barrier = pltpu.get_barrier_semaphore()
    near = [tdev(1), tdev(2), tdev(3), xp, xm, yp, ym, yo, mate]
    for device in near:
        pl.semaphore_signal(barrier, inc=1, device_id=device, device_id_type=MESH)

    @pl.when(up_edge)
    def _():
        pl.semaphore_signal(barrier, inc=1, device_id=up1, device_id_type=MESH)

    @pl.when(down_edge)
    def _():
        pl.semaphore_signal(barrier, inc=1, device_id=down1, device_id_type=MESH)

    edge = up_edge.astype(jnp.int32) + down_edge.astype(jnp.int32)
    pl.semaphore_wait(barrier, len(near) + edge)

    @pl.when(up_edge)
    def _():
        pl.semaphore_signal(go, inc=1, device_id=up1, device_id_type=MESH)

    @pl.when(down_edge)
    def _():
        pl.semaphore_signal(go, inc=1, device_id=down1, device_id_type=MESH)

    net = Links(ssem, rsem)

    lp.wait()
    tile = pb.at[c, y, z]
    pz = [net.send(tile, tile, tdev(k)) for k in (2, 1, 3)]

    def block_set(b):
        b = (b + 4) % 4
        return pb.at[c, y, pl.ds(pl.multiple_of(4 * b, 4), 4)]

    def relay(up, j, k):
        moved = block_set(zh - j if up else zh + j)
        return pltpu.make_async_remote_copy(
            src_ref=moved,
            dst_ref=moved,
            send_sem=psem.at[(0 if up else 12) + 4 * j + k - 1],
            recv_sem=qsem.at[(0 if up else 3) + j],
            device_id=zdev(k if up else -k),
            device_id_type=MESH,
        )

    def relay_start(up, j):
        here = (up_edge & (zh >= j)) if up else (down_edge & (zh + j <= 3))

        @pl.when(here)
        def _():
            if j == 0:
                pl.semaphore_wait(go, 1)
            for k in (4, 3, 2, 1):
                relay(up, j, k).start()

    def relay_sent(up, j):
        here = (up_edge & (zh >= j)) if up else (down_edge & (zh + j <= 3))

        @pl.when(here)
        def _():
            for k in (4, 3, 2, 1):
                relay(up, j, k).wait_send()

    def relay_arrived(up, j):
        here = (zh >= j + 1) if up else (zh + j + 1 <= 3)

        @pl.when(here)
        def _():
            relay(up, j, 1).wait_recv()

    def relay_step(j):
        for up in (True, False):
            relay_arrived(up, j)
            if j < 2:
                relay_start(up, j + 1)

    lq.wait()
    pa = []
    for k in (2, 1, 3):
        src = A.at[0, rows_a(x, y), :]
        pa.append(net.send(src, A.at[4 - k, rows_a(x, y), :], tdev(k)))
    for copy in lo:
        copy.wait()
    pbq = []
    for k in (2, 1, 3):
        src = B.at[0, rows_b(), cols_b(x, y)]
        pbq.append(net.send(src, B.at[4 - k, rows_b(), cols_b(x, y)], tdev(k)))

    ls.wait()
    st = []
    for cc in range(2):
        part = []
        for k in (2, 1, 3):
            peer = (t + k) % 4
            src = xs.at[pl.ds(pl.multiple_of(256 * peer + 128 * cc, 128), 128), :]
            dst = xb.at[t, pl.ds(128 * cc, 128), :]
            part.append(net.send(src, dst, tdev(k)))
        st.append(part)

    for copy in pa:
        copy.wait_recv()
    own_a, own_b = slice_a(x, y), slice_b(x, y)
    a_xp = net.send(own_a, own_a, xp)
    a_xm = net.send(own_a, own_a, xm)
    for copy in pbq:
        copy.wait_recv()
    b_yp = net.send(own_b, own_b, yp)
    b_ym = net.send(own_b, own_b, ym)
    ya = {0: (net.send(own_a, own_a, yp), net.send(own_a, own_a, ym))}
    xbp = {0: (net.send(own_b, own_b, xp), net.send(own_b, own_b, xm))}

    for copy in pz:
        copy.wait_recv()
    relay_start(True, 0)
    relay_start(False, 0)

    a_xp.wait_recv()
    h = slice_a(m4(x - 1), y, 0, 32)
    a_xp2 = net.send(h, h, xp)
    s = slice_a(m4(x - 1), y)
    ya[-1] = (net.send(s, s, yp), net.send(s, s, ym))
    a_xm.wait_recv()
    h = slice_a(m4(x + 1), y, 32, 32)
    a_xm2 = net.send(h, h, xm)
    s = slice_a(m4(x + 1), y)
    ya[1] = (net.send(s, s, yp), net.send(s, s, ym))
    b_yp.wait_recv()
    h = slice_b(x, m4(y - 1), 0, 96)
    b_yp2 = net.send(h, h, yp)
    s = slice_b(x, m4(y - 1))
    xbp[-1] = (net.send(s, s, xp), net.send(s, s, xm))
    b_ym.wait_recv()
    h = slice_b(x, m4(y + 1), 96, 96)
    b_ym2 = net.send(h, h, ym)
    s = slice_b(x, m4(y + 1))
    xbp[1] = (net.send(s, s, xp), net.send(s, s, xm))

    a_xp2.wait_recv()
    a_xm2.wait_recv()
    s = slice_a(m4(x + 2), y)
    ya[2] = (net.send(s, s, yp), net.send(s, s, ym))
    b_yp2.wait_recv()
    b_ym2.wait_recv()
    s = slice_b(x, m4(y + 2))
    xbp[2] = (net.send(s, s, xp), net.send(s, s, xm))

    def set_a(yy):
        return A.at[1:4, pl.ds(pl.multiple_of(64 * (c * 16 + yy * 4), 256), 256), :]

    def set_b(xx):
        return B.at[1:4, rows_b(), pl.ds(pl.multiple_of(512 * xx, 512), 512)]

    relay_step(0)
    mates = [net.send(set_a(y), set_a(y), mate), net.send(set_b(x), set_b(x), mate)]

    fwd = {}
    for dx in (0, -1, 1, 2):
        ya[dx][0].wait_recv()
        h = slice_a(m4(x + dx), m4(y - 1), 0, 32)
        f0 = net.send(h, h, yp)
        ya[dx][1].wait_recv()
        h = slice_a(m4(x + dx), m4(y + 1), 32, 32)
        f1 = net.send(h, h, ym)
        xbp[dx][0].wait_recv()
        h = slice_b(m4(x - 1), m4(y + dx), 0, 96)
        f2 = net.send(h, h, xp)
        xbp[dx][1].wait_recv()
        h = slice_b(m4(x + 1), m4(y + dx), 96, 96)
        f3 = net.send(h, h, xm)
        fwd[dx] = (f0, f1, f2, f3)
        if dx == -1:
            relay_step(1)
    relay_step(2)
    line = pb.at[c, y]
    py = [net.send(line, line, d) for d in (yo, yp, ym)]
    for s in (set_a(m4(y - 1)), set_a(m4(y + 1)), set_b(m4(x - 1)), set_b(m4(x + 1))):
        mates.append(net.send(s, s, mate))
    for copy in py:
        copy.wait_recv()
    pm = net.send(pb.at[c], pb.at[c], mate)

    lx.wait()
    for copy in small:
        copy.wait()

    def norm_cand(cc):
        rows = pl.ds(128 * cc, 128)
        into = pl.ds(NPRE + 128 * cc, 128)
        total = jnp.zeros((128, 1), F32)
        for f in range(4):
            v = xb[f, rows, :].astype(F32)
            total += jnp.sum(v * v, axis=-1, keepdims=True)
        scale = lax.rsqrt(total * (1.0 / D) + EPS)
        for f in range(4):
            v = xb[f, rows, :].astype(F32)
            g = gain[:, FC * f : FC * (f + 1)]
            xn[into, FC * f : FC * (f + 1)] = (v * scale * g).astype(BF16)

    for copy in st[0]:
        copy.wait_recv()
    norm_cand(0)

    for dx in (0, -1, 1, 2):
        f0, f1, f2, f3 = fwd[dx]
        f0.wait_recv()
        f1.wait_recv()
        s = slice_a(m4(x + dx), m4(y + 2))
        mates.append(net.send(s, s, mate))
        f2.wait_recv()
        f3.wait_recv()
        s = slice_b(m4(x + 2), m4(y + dx))
        mates.append(net.send(s, s, mate))

    pm.wait_recv()
    for f in range(4):
        for g in range(32):
            pf[f, 2 * g : 2 * g + 2, :] = pb[g // 16, (g // 4) % 4, (g % 4) * 4 + f].astype(F32)
    total = jnp.zeros((PRE, 1), F32)
    for f in range(4):
        total += jnp.sum(pf[f] * pf[f], axis=-1, keepdims=True)
    scale = lax.rsqrt(total * (1.0 / D) + EPS)
    for f in range(4):
        g = gain[:, FC * f : FC * (f + 1)]
        xn[0:PRE, FC * f : FC * (f + 1)] = (pf[f] * scale * g).astype(BF16)

    for copy in mates:
        copy.wait_recv()

    def rotate(v, cos, sin):
        a, b = v[:, :128], v[:, 128:]
        return jnp.concatenate([a * cos - b * sin, b * cos + a * sin], axis=-1)

    def project_kv(start, n, first):
        xv = xn[start : start + n, :]
        for pair in range(2):
            w = jnp.concatenate([B[2 * pair, 256:384, :], B[2 * pair + 1, 256:384, :]], axis=0)
            r = lax.dot_general(xv, w, (((1,), (1,)), ((), ())), preferred_element_type=F32)
            kvs[2 * pair, 0:n, :] = r[:, :128]
            kvs[2 * pair + 1, 0:n, :] = r[:, 128:]
        parts = [kvs[(f - t + 4) % 4, 0:n, :] for f in range(4)]
        key = jnp.concatenate([p[:, :64] for p in parts], axis=-1)
        val = jnp.concatenate([p[:, 64:] for p in parts], axis=-1)
        into = pl.ds(first, n)
        kc[into, :] = rotate(key, cos_t[into, :], sin_t[into, :]).astype(BF16)
        vc[into, :] = val.astype(BF16)

    outs = []
    for cc in range(2):
        rows = pl.ds(128 * cc, 128)
        xrows = pl.ds(NPRE + 128 * cc, 128)
        if cc == 0:
            project_kv(0, PRE + CL, 0)
        else:
            for copy in st[1]:
                copy.wait_recv()
            norm_cand(1)
            project_kv(PRE + CL, CL, PRE)

        def head(r, carry, xrows=xrows):
            qv = jnp.dot(xn[xrows, :], A[r], preferred_element_type=F32)
            qv = rotate(qv, cos_t[PRE:, :], sin_t[PRE:, :]) * (HS ** -0.5)
            q4[pl.ds(pl.multiple_of(r * CL, CL), CL), :] = qv.astype(BF16)
            return carry

        lax.fori_loop(0, 4, head, 0)
        live = lens[2 * t + cc]

        scores = lax.dot_general(
            q4[...], kc[...], (((1,), (1,)), ((), ())), preferred_element_type=F32
        )
        row = lax.broadcasted_iota(jnp.int32, scores.shape, 0) % CL
        col = lax.broadcasted_iota(jnp.int32, scores.shape, 1)
        scores = jnp.where(col <= row + PRE, scores, -jnp.inf)
        weights = jnp.exp(scores - jnp.max(scores, axis=-1, keepdims=True))
        divisor = jnp.sum(weights, axis=-1, keepdims=True)
        mix = jnp.dot(weights.astype(BF16), vc[...], preferred_element_type=F32) / divisor
        slot = lax.broadcasted_iota(jnp.int32, mix.shape, 0) % CL
        hr[...] = jnp.where(slot < live, mix, 0.0).astype(BF16)

        def out_cols(n, carry, rows=rows):
            cols = pl.ds(pl.multiple_of(n * 512, 512), 512)
            acc = jnp.zeros((CL, 512), F32)
            for r in range(4):
                acc += jnp.dot(
                    hr[r * CL : (r + 1) * CL, :], B[r, 0:256, cols], preferred_element_type=F32
                )
            ob[rows, cols] = acc.astype(BF16)
            return carry

        lax.fori_loop(0, 4, out_cols, 0)
        outs.append(local(11 + cc, ob.at[rows, :], out.at[rows, :]))

    net.finish()
    for up in (True, False):
        for j in range(3):
            relay_sent(up, j)
    for copy in outs:
        copy.wait()


def body(cand_states, prefix_states, norm_gain, w_query, w_key, w_value, w_out, cand_lengths):
    cos_np, sin_np = rope_tables()
    any_spec = pl.BlockSpec(memory_space=pl.ANY)
    return pl.pallas_call(
        kernel,
        out_shape=jax.ShapeDtypeStruct((256, D), BF16),
        in_specs=[any_spec] * 10,
        out_specs=any_spec,
        scratch_shapes=[
            pltpu.VMEM((4, D, HS), BF16),
            pltpu.VMEM((4, 384, D), BF16),
            pltpu.VMEM((1024, FC), BF16),
            pltpu.VMEM((4, 256, FC), BF16),
            pltpu.VMEM((2, 4, 16, 2, FC), BF16),
            pltpu.VMEM((4, PRE, FC), F32),
            pltpu.VMEM((320, D), BF16),
            pltpu.VMEM((4, PRE + CL, 128), F32),
            pltpu.VMEM((CL + PRE, HS), BF16),
            pltpu.VMEM((CL + PRE, HS), BF16),
            pltpu.VMEM((4 * CL, HS), BF16),
            pltpu.VMEM((4 * CL, HS), BF16),
            pltpu.VMEM((256, D), BF16),
            pltpu.VMEM((1, D), F32),
            pltpu.VMEM((PRE + CL, 128), F32),
            pltpu.VMEM((PRE + CL, 128), F32),
            pltpu.SMEM((8,), jnp.int32),
            pltpu.SemaphoreType.DMA((N_SEMS,)),
            pltpu.SemaphoreType.DMA((N_SEMS,)),
            pltpu.SemaphoreType.DMA((16,)),
            pltpu.SemaphoreType.DMA((24,)),
            pltpu.SemaphoreType.DMA((6,)),
            pltpu.SemaphoreType.REGULAR,
        ],
        compiler_params=pltpu.CompilerParams(
            collective_id=0, has_side_effects=True, vmem_limit_bytes=56 * 1024 * 1024
        ),
        name="sublayer",
    )(
        cand_states, prefix_states, norm_gain.reshape(1, D), w_query, w_key.T, w_value.T,
        w_out, cand_lengths, jnp.asarray(cos_np), jnp.asarray(sin_np),
    )


def solution(mesh):
    in_specs = (
        P(("query", "cand"), "tensor"),
        P(("query", "cand"), "tensor"),
        P(),
        P(None, "tensor"),
        P(None, "tensor"),
        P(None, "tensor"),
        P("tensor", None),
        P(("query", "cand")),
    )
    out_specs = P(("query", "cand", "tensor"), None)
    return jax.shard_map(body, mesh=mesh, in_specs=in_specs, out_specs=out_specs, check_vma=False)
```

```python
import numpy as np

import jax
import jax.numpy as jnp
from jax import lax
from jax.experimental import pallas as pl
from jax.experimental.pallas import tpu as pltpu
from jax.sharding import PartitionSpec as P

MESH = pl.DeviceIdType.MESH
BF16 = jnp.bfloat16
F32 = jnp.float32
EPS = 1e-06
THETA = 10000.0

NX = 4
NY = 4
NZ = 16
ZL = 4
CL = 128
HS = 256
D = 2048
FC = 512
PRE = 64


def rope_tables():
    half = HS // 2
    freq = (THETA ** (-np.arange(half, dtype=np.float32) * 2.0 / HS)).astype(np.float32)
    cand = (PRE + np.arange(CL)).astype(np.float32)
    core, y, zh, r = np.meshgrid(
        np.arange(2), np.arange(4), np.arange(4), np.arange(2), indexing="ij"
    )
    pre = ((zh * 8 + y * 2 + core) * 2 + r).reshape(-1).astype(np.float32)
    pos = np.concatenate([pre, cand])
    angles = (pos[:, None] * freq[None, :]).astype(np.float32).astype(np.float64)
    return np.cos(angles).astype(np.float32), np.sin(angles).astype(np.float32)


class Links:
    def __init__(self, ssem, rsem):
        self.ssem, self.rsem, self.made = ssem, rsem, []

    def send(self, src, dst, device):
        i = len(self.made)
        copy = pltpu.make_async_remote_copy(
            src_ref=src,
            dst_ref=dst,
            send_sem=self.ssem.at[i],
            recv_sem=self.rsem.at[i],
            device_id=device,
            device_id_type=MESH,
        )
        copy.start()
        self.made.append(copy)
        return copy

    def finish(self):
        for copy in self.made:
            copy.wait_send()


N_SEMS = 136
NPRE = PRE


def kernel(
    states, prefix, gain_h, wq, wk, wv, wo, lens_h, cos_h, sin_h,
    out,
    A, B, xs, xb, pb, pf, xn, kvs, kc, vc, q4, hr, ob, gain, cos_t, sin_t, lens,
    ssem, rsem, lsem, psem, qsem, go, chain, go_dn, chain_dn,
):
    x = lax.axis_index("query")
    cd = lax.axis_index("cand")
    t = lax.axis_index("tensor")
    zh = cd // 8
    y = (cd // 2) % 4
    c = cd % 2
    z = zh * 4 + t

    def at(xx, yy, zz, cc):
        return (xx, (zz // 4) * 8 + yy * 2 + cc, zz % 4)

    def m4(v):
        return (v + 8) % 4

    def zdev(dz):
        return at(x, y, (z + dz + 32) % 16, c)

    def tdev(k):
        return (x, cd, (t + k) % 4)

    xp, xm = at(m4(x + 1), y, z, c), at(m4(x - 1), y, z, c)
    yp, ym = at(x, m4(y + 1), z, c), at(x, m4(y - 1), z, c)
    yo = at(x, m4(y + 2), z, c)
    mate = at(x, y, z, 1 - c)

    def part_a(s, first, second, off=0, n=32, q=slice(1, 4)):
        row = c * 1024 + s * 512 + 32 * (second * 4 + first) + off
        return A.at[q, pl.ds(pl.multiple_of(row, 16), n), :]

    def part_b(s, first, second, off=0, n=96, q=slice(1, 4)):
        row = 192 * c + 96 * s + off
        col = 128 * (second * 4 + first)
        return B.at[
            q, pl.ds(pl.multiple_of(row, 16), n), pl.ds(pl.multiple_of(col, 128), 128)
        ]

    def set_a(s, second):
        row = c * 1024 + s * 512 + 128 * second
        return A.at[1:4, pl.ds(pl.multiple_of(row, 128), 128), :]

    def set_b(s, second):
        row, col = 192 * c + 96 * s, 512 * second
        return B.at[
            1:4, pl.ds(pl.multiple_of(row, 32), 96), pl.ds(pl.multiple_of(col, 512), 512)
        ]

    def local(i, src, dst):
        copy = pltpu.make_async_copy(src, dst, lsem.at[i])
        copy.start()
        return copy

    lp = local(0, prefix, pb.at[c, y, z])
    lq = local(1, wq, A.at[0])
    lo = [
        local(2, wk, B.at[0, 256:320, :]),
        local(3, wv, B.at[0, 320:384, :]),
        local(4, wo, B.at[0, 0:256, :]),
    ]
    ls = local(5, states, xs)
    lx = local(6, states.at[pl.ds(pl.multiple_of(256 * t, 256), 256), :], xb.at[t])
    small = [
        local(7, gain_h, gain),
        local(8, cos_h, cos_t),
        local(9, sin_h, sin_t),
        local(10, lens_h, lens),
    ]

    up_edge = (t == 3) & (zh < 3)
    down_edge = (t == 0) & (zh > 0)
    up1, down1 = zdev(1), zdev(-1)
    barrier = pltpu.get_barrier_semaphore()
    near = [tdev(1), tdev(2), tdev(3), xp, xm, yp, ym, yo, mate]
    for device in near:
        pl.semaphore_signal(barrier, inc=1, device_id=device, device_id_type=MESH)

    @pl.when(up_edge)
    def _():
        pl.semaphore_signal(barrier, inc=1, device_id=up1, device_id_type=MESH)

    @pl.when(down_edge)
    def _():
        pl.semaphore_signal(barrier, inc=1, device_id=down1, device_id_type=MESH)

    edge = up_edge.astype(jnp.int32) + down_edge.astype(jnp.int32)
    pl.semaphore_wait(barrier, len(near) + edge)

    @pl.when(down_edge)
    def _():
        @pl.when(zh == 3)
        def _():
            pl.semaphore_signal(go_dn, inc=1, device_id=down1, device_id_type=MESH)

        pl.semaphore_wait(go, 1)
        pl.semaphore_signal(chain, inc=1, device_id=tdev(3), device_id_type=MESH)

    @pl.when(up_edge)
    def _():
        @pl.when(zh > 0)
        def _():
            pl.semaphore_wait(chain, 1)

        pl.semaphore_signal(go, inc=1, device_id=up1, device_id_type=MESH)

    @pl.when((t == 3) & (zh == 3))
    def _():
        pl.semaphore_wait(chain, 1)

    net = Links(ssem, rsem)

    lp.wait()
    tile = pb.at[c, y, z]
    pz = [net.send(tile, tile, tdev(k)) for k in (2, 1, 3)]

    def block_set(b):
        b = (b + 4) % 4
        return pb.at[c, y, pl.ds(pl.multiple_of(4 * b, 4), 4)]

    def spread(k):
        moved = block_set(zh)
        far = 1 if abs(k) > 4 else (2 if k > 0 else 0)
        return pltpu.make_async_remote_copy(
            src_ref=moved,
            dst_ref=moved,
            send_sem=psem.at[k - 1 if k > 0 else 5 - k],
            recv_sem=qsem.at[far],
            device_id=zdev(k),
            device_id_type=MESH,
        )

    ways = ((3, (6, 5, 4, 3, 2, 1)), (0, (-6, -5, -4, -3, -2, -1)))

    def spread_from(end):
        for k in ways[0][1] if end == 3 else ways[1][1]:
            spread(k).start()

    def heard_above(b):
        @pl.when((t == 3) & (zh == b))
        def _():
            pl.semaphore_wait(go_dn, 1)
            pl.semaphore_signal(chain_dn, inc=1, device_id=tdev(1), device_id_type=MESH)
            spread_from(3)

    def pass_down(b):
        @pl.when((t == 0) & (zh == b))
        def _():
            pl.semaphore_wait(chain_dn, 1)
            if b > 0:
                pl.semaphore_signal(go_dn, inc=1, device_id=down1, device_id_type=MESH)
            if b < 2:
                spread_from(0)

    def slices(part, q=slice(1, 4)):
        return part(0, x, y, q=q), part(1, y, x, q=q)

    def to_peers(part):
        sent = []
        for k in (2, 1, 3):
            for src, dst in zip(slices(part, 0), slices(part, 4 - k)):
                sent.append(net.send(src, dst, tdev(k)))
        return sent

    lq.wait()
    pa = to_peers(part_a)
    for copy in lo:
        copy.wait()
    pbq = to_peers(part_b)

    ls.wait()
    st = []
    for cc in range(2):
        part = []
        for k in (2, 1, 3):
            peer = (t + k) % 4
            src = xs.at[pl.ds(pl.multiple_of(256 * peer + 128 * cc, 128), 128), :]
            dst = xb.at[t, pl.ds(128 * cc, 128), :]
            part.append(net.send(src, dst, tdev(k)))
        st.append(part)

    mates = []

    class Stream:
        def __init__(self, part, whole, s, n):
            self.part = lambda i, j, off=0, n=n: part(s, m4(self.me[0] + i), m4(self.me[1] + j), off, n)
            self.whole = lambda j: whole(s, m4(self.me[1] + j))
            self.me = (x, y) if s == 0 else (y, x)
            self.first = (xp, xm) if s == 0 else (yp, ym)
            self.second = (yp, ym) if s == 0 else (xp, xm)
            self.half = n // 2
            self.onward = {}

        def both(self, piece, dirs):
            return tuple(net.send(piece, piece, d) for d in dirs)

        def own(self):
            piece = self.part(0, 0)
            self.near_copies = self.both(piece, self.first)
            self.onward[0] = self.both(piece, self.second)

        def near(self):
            self.far_copies = []
            for side, i in ((0, -1), (1, 1)):
                self.near_copies[side].wait_recv()
                h = self.part(i, 0, side * self.half, self.half)
                self.far_copies.append(net.send(h, h, self.first[side]))
                self.onward[i] = self.both(self.part(i, 0), self.second)

        def far(self):
            for copy in self.far_copies:
                copy.wait_recv()
            self.onward[2] = self.both(self.part(2, 0), self.second)
            mates.append(net.send(self.whole(0), self.whole(0), mate))

        def turn(self, i):
            self.last = getattr(self, "last", {})
            self.last[i] = []
            for side, j in ((0, -1), (1, 1)):
                self.onward[i][side].wait_recv()
                h = self.part(i, j, side * self.half, self.half)
                self.last[i].append(net.send(h, h, self.second[side]))
            if i == 2:
                for j in (-1, 1):
                    mates.append(net.send(self.whole(j), self.whole(j), mate))

        def end(self, i):
            for copy in self.last[i]:
                copy.wait_recv()
            s = self.part(i, 2)
            mates.append(net.send(s, s, mate))

    sa = [Stream(part_a, set_a, s, 32) for s in (0, 1)]
    sb = [Stream(part_b, set_b, s, 96) for s in (0, 1)]
    for copy in pa:
        copy.wait_recv()
    for w in sa:
        w.own()
    for copy in pz:
        copy.wait_recv()
    @pl.when((t == 3) & (zh == 3))
    def _():
        spread_from(3)

    @pl.when((t == 0) & (zh >= 2))
    def _():
        spread_from(0)

    heard_above(2)
    for w in sa:
        w.near()
    pass_down(2)
    for copy in pbq:
        copy.wait_recv()
    for w in sb:
        w.own()
    for w in sa:
        w.far()
    heard_above(1)
    pass_down(1)
    for i in (0, -1, 1, 2):
        for w in sa:
            w.turn(i)
        if i == -1:
            for w in sb:
                w.near()
            heard_above(0)
            pass_down(0)
    for w in sb:
        w.far()
    for i in (0, -1, 1, 2):
        for w in sb:
            w.turn(i)
        for w in sa:
            w.end(i)
    a_mates, mates = mates, []

    for k in (-1, 5, 1):
        spread(k).wait_recv()
    line = pb.at[c, y]
    py = [net.send(line, line, d) for d in (yo, yp, ym)]

    lx.wait()
    for copy in small:
        copy.wait()

    def norm_cand(cc):
        rows = pl.ds(128 * cc, 128)
        into = pl.ds(NPRE + 128 * cc, 128)
        total = jnp.zeros((128, 1), F32)
        for f in range(4):
            v = xb[f, rows, :].astype(F32)
            total += jnp.sum(v * v, axis=-1, keepdims=True)
        scale = lax.rsqrt(total * (1.0 / D) + EPS)
        for f in range(4):
            v = xb[f, rows, :].astype(F32)
            g = gain[:, FC * f : FC * (f + 1)]
            xn[into, FC * f : FC * (f + 1)] = (v * scale * g).astype(BF16)

    for copy in st[0]:
        copy.wait_recv()
    norm_cand(0)

    for copy in a_mates:
        copy.wait_recv()

    def rotate(v, cos, sin):
        a, b = v[:, :128], v[:, 128:]
        return jnp.concatenate([a * cos - b * sin, b * cos + a * sin], axis=-1)

    def project_q(cc):
        xrows = pl.ds(NPRE + 128 * cc, 128)

        def head(r, carry):
            qv = jnp.dot(xn[xrows, :], A[r], preferred_element_type=F32)
            qv = rotate(qv, cos_t[PRE:, :], sin_t[PRE:, :]) * (HS ** -0.5)
            q4[pl.ds(pl.multiple_of(r * CL, CL), CL), :] = qv.astype(BF16)
            return carry

        lax.fori_loop(0, 4, head, 0)

    for copy in py:
        copy.wait_recv()
    pm = net.send(pb.at[c], pb.at[c], mate)
    project_q(0)

    for i in (0, -1, 1, 2):
        for w in sb:
            w.end(i)

    pm.wait_recv()
    for f in range(4):
        for g in range(32):
            pf[f, 2 * g : 2 * g + 2, :] = pb[g // 16, (g // 4) % 4, (g % 4) * 4 + f].astype(F32)
    total = jnp.zeros((PRE, 1), F32)
    for f in range(4):
        total += jnp.sum(pf[f] * pf[f], axis=-1, keepdims=True)
    scale = lax.rsqrt(total * (1.0 / D) + EPS)
    for f in range(4):
        g = gain[:, FC * f : FC * (f + 1)]
        xn[0:PRE, FC * f : FC * (f + 1)] = (pf[f] * scale * g).astype(BF16)

    for copy in mates:
        copy.wait_recv()

    def project_kv(start, n, first):
        xv = xn[start : start + n, :]
        for pair in range(2):
            w = jnp.concatenate([B[2 * pair, 256:384, :], B[2 * pair + 1, 256:384, :]], axis=0)
            r = lax.dot_general(xv, w, (((1,), (1,)), ((), ())), preferred_element_type=F32)
            kvs[2 * pair, 0:n, :] = r[:, :128]
            kvs[2 * pair + 1, 0:n, :] = r[:, 128:]
        parts = [kvs[(f - t + 4) % 4, 0:n, :] for f in range(4)]
        key = jnp.concatenate([p[:, :64] for p in parts], axis=-1)
        val = jnp.concatenate([p[:, 64:] for p in parts], axis=-1)
        into = pl.ds(first, n)
        kc[into, :] = rotate(key, cos_t[into, :], sin_t[into, :]).astype(BF16)
        vc[into, :] = val.astype(BF16)

    outs = []
    for cc in range(2):
        rows = pl.ds(128 * cc, 128)
        if cc == 0:
            project_kv(0, PRE + CL, 0)
        else:
            for copy in st[1]:
                copy.wait_recv()
            norm_cand(1)
            project_kv(PRE + CL, CL, PRE)
            project_q(1)

        live = lens[2 * t + cc]

        scores = lax.dot_general(
            q4[...], kc[...], (((1,), (1,)), ((), ())), preferred_element_type=F32
        )
        row = lax.broadcasted_iota(jnp.int32, scores.shape, 0) % CL
        col = lax.broadcasted_iota(jnp.int32, scores.shape, 1)
        scores = jnp.where(col <= row + PRE, scores, -jnp.inf)
        weights = jnp.exp(scores - jnp.max(scores, axis=-1, keepdims=True))
        divisor = jnp.sum(weights, axis=-1, keepdims=True)
        mix = jnp.dot(weights.astype(BF16), vc[...], preferred_element_type=F32) / divisor
        slot = lax.broadcasted_iota(jnp.int32, mix.shape, 0) % CL
        hr[...] = jnp.where(slot < live, mix, 0.0).astype(BF16)

        def out_cols(n, carry, rows=rows):
            cols = pl.ds(pl.multiple_of(n * 512, 512), 512)
            acc = jnp.zeros((CL, 512), F32)
            for r in range(4):
                acc += jnp.dot(
                    hr[r * CL : (r + 1) * CL, :], B[r, 0:256, cols], preferred_element_type=F32
                )
            ob[rows, cols] = acc.astype(BF16)
            return carry

        lax.fori_loop(0, 4, out_cols, 0)
        outs.append(local(11 + cc, ob.at[rows, :], out.at[rows, :]))

    net.finish()
    for end, ks in ways:
        @pl.when(t == end)
        def _(ks=ks):
            for k in ks:
                spread(k).wait_send()

    for copy in outs:
        copy.wait()


def body(cand_states, prefix_states, norm_gain, w_query, w_key, w_value, w_out, cand_lengths):
    cos_np, sin_np = rope_tables()
    any_spec = pl.BlockSpec(memory_space=pl.ANY)
    return pl.pallas_call(
        kernel,
        out_shape=jax.ShapeDtypeStruct((256, D), BF16),
        in_specs=[any_spec] * 10,
        out_specs=any_spec,
        scratch_shapes=[
            pltpu.VMEM((4, D, HS), BF16),
            pltpu.VMEM((4, 384, D), BF16),
            pltpu.VMEM((1024, FC), BF16),
            pltpu.VMEM((4, 256, FC), BF16),
            pltpu.VMEM((2, 4, 16, 2, FC), BF16),
            pltpu.VMEM((4, PRE, FC), F32),
            pltpu.VMEM((320, D), BF16),
            pltpu.VMEM((4, PRE + CL, 128), F32),
            pltpu.VMEM((CL + PRE, HS), BF16),
            pltpu.VMEM((CL + PRE, HS), BF16),
            pltpu.VMEM((4 * CL, HS), BF16),
            pltpu.VMEM((4 * CL, HS), BF16),
            pltpu.VMEM((256, D), BF16),
            pltpu.VMEM((1, D), F32),
            pltpu.VMEM((PRE + CL, 128), F32),
            pltpu.VMEM((PRE + CL, 128), F32),
            pltpu.SMEM((8,), jnp.int32),
            pltpu.SemaphoreType.DMA((N_SEMS,)),
            pltpu.SemaphoreType.DMA((N_SEMS,)),
            pltpu.SemaphoreType.DMA((16,)),
            pltpu.SemaphoreType.DMA((12,)),
            pltpu.SemaphoreType.DMA((3,)),
            pltpu.SemaphoreType.REGULAR,
            pltpu.SemaphoreType.REGULAR,
            pltpu.SemaphoreType.REGULAR,
            pltpu.SemaphoreType.REGULAR,
        ],
        compiler_params=pltpu.CompilerParams(
            collective_id=0, has_side_effects=True, vmem_limit_bytes=56 * 1024 * 1024
        ),
        name="sublayer",
    )(
        cand_states, prefix_states, norm_gain.reshape(1, D), w_query, w_key.T, w_value.T,
        w_out, cand_lengths, jnp.asarray(cos_np), jnp.asarray(sin_np),
    )


def solution(mesh):
    in_specs = (
        P(("query", "cand"), "tensor"),
        P(("query", "cand"), "tensor"),
        P(),
        P(None, "tensor"),
        P(None, "tensor"),
        P(None, "tensor"),
        P("tensor", None),
        P(("query", "cand")),
    )
    out_specs = P(("query", "cand", "tensor"), None)
    return jax.shard_map(body, mesh=mesh, in_specs=in_specs, out_specs=out_specs, check_vma=False)
```

```python
import numpy as np

import jax
import jax.numpy as jnp
from jax import lax
from jax.experimental import pallas as pl
from jax.experimental.pallas import tpu as pltpu
from jax.sharding import PartitionSpec as P

MESH = pl.DeviceIdType.MESH
BF16 = jnp.bfloat16
F32 = jnp.float32
EPS = 1e-06
THETA = 10000.0

NX = 4
NY = 4
NZ = 16
ZL = 4
CL = 128
HS = 256
D = 2048
FC = 512
PRE = 64


def rope_tables():
    half = HS // 2
    freq = (THETA ** (-np.arange(half, dtype=np.float32) * 2.0 / HS)).astype(np.float32)
    cand = (PRE + np.arange(CL)).astype(np.float32)
    core, y, zh, r = np.meshgrid(
        np.arange(2), np.arange(4), np.arange(4), np.arange(2), indexing="ij"
    )
    pre = ((zh * 8 + y * 2 + core) * 2 + r).reshape(-1).astype(np.float32)
    pos = np.concatenate([pre, cand])
    angles = (pos[:, None] * freq[None, :]).astype(np.float32).astype(np.float64)
    return np.cos(angles).astype(np.float32), np.sin(angles).astype(np.float32)


class Links:
    def __init__(self, ssem, rsem):
        self.ssem, self.rsem, self.made = ssem, rsem, []

    def send(self, src, dst, device):
        i = len(self.made)
        copy = pltpu.make_async_remote_copy(
            src_ref=src,
            dst_ref=dst,
            send_sem=self.ssem.at[i],
            recv_sem=self.rsem.at[i],
            device_id=device,
            device_id_type=MESH,
        )
        copy.start()
        self.made.append(copy)
        return copy

    def finish(self):
        for copy in self.made:
            copy.wait_send()


N_SEMS = 136
NPRE = PRE


def kernel(
    states, prefix, gain_h, wq, wk, wv, wo, lens_h, cos_h, sin_h,
    out,
    A, B, xs, xb, pb, pf, xn, kvs, kc, vc, q4, hr, ob, gain, cos_t, sin_t, lens,
    ssem, rsem, lsem, psem, qsem, go, chain, go_dn, chain_dn,
):
    x = lax.axis_index("query")
    cd = lax.axis_index("cand")
    t = lax.axis_index("tensor")
    zh = cd // 8
    y = (cd // 2) % 4
    c = cd % 2
    z = zh * 4 + t

    def at(xx, yy, zz, cc):
        return (xx, (zz // 4) * 8 + yy * 2 + cc, zz % 4)

    def m4(v):
        return (v + 8) % 4

    def zdev(dz):
        return at(x, y, (z + dz + 32) % 16, c)

    def tdev(k):
        return (x, cd, (t + k) % 4)

    xp, xm = at(m4(x + 1), y, z, c), at(m4(x - 1), y, z, c)
    yp, ym = at(x, m4(y + 1), z, c), at(x, m4(y - 1), z, c)
    yo = at(x, m4(y + 2), z, c)
    mate = at(x, y, z, 1 - c)

    def part_a(s, first, second, off=0, n=32, q=slice(1, 4)):
        row = c * 1024 + s * 512 + 32 * (second * 4 + first) + off
        return A.at[q, pl.ds(pl.multiple_of(row, 16), n), :]

    def part_b(s, first, second, off=0, n=96, q=slice(1, 4)):
        row = 192 * c + 96 * s + off
        col = 128 * (second * 4 + first)
        return B.at[
            q, pl.ds(pl.multiple_of(row, 16), n), pl.ds(pl.multiple_of(col, 128), 128)
        ]

    def set_a(s, second):
        row = c * 1024 + s * 512 + 128 * second
        return A.at[1:4, pl.ds(pl.multiple_of(row, 128), 128), :]

    def set_b(s, second):
        row, col = 192 * c + 96 * s, 512 * second
        return B.at[
            1:4, pl.ds(pl.multiple_of(row, 32), 96), pl.ds(pl.multiple_of(col, 512), 512)
        ]

    def local(i, src, dst):
        copy = pltpu.make_async_copy(src, dst, lsem.at[i])
        copy.start()
        return copy

    lp = local(0, prefix, pb.at[c, y, z])
    lq = local(1, wq, A.at[0])
    lo = [
        local(2, wk, B.at[0, 256:320, :]),
        local(3, wv, B.at[0, 320:384, :]),
        local(4, wo, B.at[0, 0:256, :]),
    ]
    ls = local(5, states, xs)
    lx = local(6, states.at[pl.ds(pl.multiple_of(256 * t, 256), 256), :], xb.at[t])
    small = [
        local(7, gain_h, gain),
        local(8, cos_h, cos_t),
        local(9, sin_h, sin_t),
        local(10, lens_h, lens),
    ]

    up_edge = (t == 3) & (zh < 3)
    down_edge = (t == 0) & (zh > 0)
    up1, down1 = zdev(1), zdev(-1)
    barrier = pltpu.get_barrier_semaphore()
    near = [tdev(1), tdev(2), tdev(3), xp, xm, yp, ym, yo, mate]
    for device in near:
        pl.semaphore_signal(barrier, inc=1, device_id=device, device_id_type=MESH)

    @pl.when(up_edge)
    def _():
        pl.semaphore_signal(barrier, inc=1, device_id=up1, device_id_type=MESH)

    @pl.when(down_edge)
    def _():
        pl.semaphore_signal(barrier, inc=1, device_id=down1, device_id_type=MESH)

    edge = up_edge.astype(jnp.int32) + down_edge.astype(jnp.int32)
    pl.semaphore_wait(barrier, len(near) + edge)

    @pl.when(down_edge)
    def _():
        @pl.when(zh == 3)
        def _():
            pl.semaphore_signal(go_dn, inc=1, device_id=down1, device_id_type=MESH)

        pl.semaphore_wait(go, 1)
        pl.semaphore_signal(chain, inc=1, device_id=tdev(3), device_id_type=MESH)

    @pl.when(up_edge)
    def _():
        @pl.when(zh > 0)
        def _():
            pl.semaphore_wait(chain, 1)

        pl.semaphore_signal(go, inc=1, device_id=up1, device_id_type=MESH)

    @pl.when((t == 3) & (zh == 3))
    def _():
        pl.semaphore_wait(chain, 1)

    net = Links(ssem, rsem)

    lp.wait()
    tile = pb.at[c, y, z]
    pz = [net.send(tile, tile, tdev(k)) for k in (2, 1, 3)]

    def block_set(b):
        b = (b + 4) % 4
        return pb.at[c, y, pl.ds(pl.multiple_of(4 * b, 4), 4)]

    def spread(k):
        moved = block_set(zh)
        far = 1 if abs(k) > 4 else (2 if k > 0 else 0)
        return pltpu.make_async_remote_copy(
            src_ref=moved,
            dst_ref=moved,
            send_sem=psem.at[k - 1 if k > 0 else 5 - k],
            recv_sem=qsem.at[far],
            device_id=zdev(k),
            device_id_type=MESH,
        )

    ways = ((3, (6, 5, 4, 3, 2, 1)), (0, (-6, -5, -4, -3, -2, -1)))

    def spread_from(end):
        for k in ways[0][1] if end == 3 else ways[1][1]:
            spread(k).start()

    def heard_above(b):
        @pl.when((t == 3) & (zh == b))
        def _():
            pl.semaphore_wait(go_dn, 1)
            pl.semaphore_signal(chain_dn, inc=1, device_id=tdev(1), device_id_type=MESH)
            spread_from(3)

    def pass_down(b):
        @pl.when((t == 0) & (zh == b))
        def _():
            pl.semaphore_wait(chain_dn, 1)
            if b > 0:
                pl.semaphore_signal(go_dn, inc=1, device_id=down1, device_id_type=MESH)
            if b < 2:
                spread_from(0)

    def slices(part, q=slice(1, 4)):
        return part(0, x, y, q=q), part(1, y, x, q=q)

    def to_peers(part):
        sent = []
        for k in (2, 1, 3):
            for src, dst in zip(slices(part, 0), slices(part, 4 - k)):
                sent.append(net.send(src, dst, tdev(k)))
        return sent

    lq.wait()
    pa = to_peers(part_a)
    for copy in lo:
        copy.wait()
    pbq = to_peers(part_b)

    ls.wait()
    st = []
    for cc in range(2):
        part = []
        for k in (2, 1, 3):
            peer = (t + k) % 4
            src = xs.at[pl.ds(pl.multiple_of(256 * peer + 128 * cc, 128), 128), :]
            dst = xb.at[t, pl.ds(128 * cc, 128), :]
            part.append(net.send(src, dst, tdev(k)))
        st.append(part)

    mates = []

    class Stream:
        def __init__(self, part, whole, s, n):
            self.part = lambda i, j, off=0, n=n: part(s, m4(self.me[0] + i), m4(self.me[1] + j), off, n)
            self.whole = lambda j: whole(s, m4(self.me[1] + j))
            self.me = (x, y) if s == 0 else (y, x)
            self.first = (xp, xm) if s == 0 else (yp, ym)
            self.second = (yp, ym) if s == 0 else (xp, xm)
            self.half = n // 2
            self.onward = {}

        def both(self, piece, dirs):
            return tuple(net.send(piece, piece, d) for d in dirs)

        def own(self):
            piece = self.part(0, 0)
            self.near_copies = self.both(piece, self.first)
            self.onward[0] = self.both(piece, self.second)

        def near(self):
            self.far_copies = []
            for side, i in ((0, -1), (1, 1)):
                self.near_copies[side].wait_recv()
                h = self.part(i, 0, side * self.half, self.half)
                self.far_copies.append(net.send(h, h, self.first[side]))
                self.onward[i] = self.both(self.part(i, 0), self.second)

        def far(self):
            for copy in self.far_copies:
                copy.wait_recv()
            self.onward[2] = self.both(self.part(2, 0), self.second)
            mates.append(net.send(self.whole(0), self.whole(0), mate))

        def turn(self, i):
            self.last = getattr(self, "last", {})
            self.last[i] = []
            for side, j in ((0, -1), (1, 1)):
                self.onward[i][side].wait_recv()
                h = self.part(i, j, side * self.half, self.half)
                self.last[i].append(net.send(h, h, self.second[side]))
            if i == 2:
                for j in (-1, 1):
                    mates.append(net.send(self.whole(j), self.whole(j), mate))

        def end(self, i):
            for copy in self.last[i]:
                copy.wait_recv()
            s = self.part(i, 2)
            mates.append(net.send(s, s, mate))

    sa = [Stream(part_a, set_a, s, 32) for s in (0, 1)]
    sb = [Stream(part_b, set_b, s, 96) for s in (0, 1)]
    for copy in pa:
        copy.wait_recv()
    for w in sa:
        w.own()
    for copy in pz:
        copy.wait_recv()
    @pl.when((t == 3) & (zh == 3))
    def _():
        spread_from(3)

    @pl.when((t == 0) & (zh >= 2))
    def _():
        spread_from(0)

    heard_above(2)
    for w in sa:
        w.near()
    pass_down(2)
    for copy in pbq:
        copy.wait_recv()
    for w in sb:
        w.own()
    for w in sa:
        w.far()
    heard_above(1)
    pass_down(1)
    for i in (0, -1, 1, 2):
        for w in sa:
            w.turn(i)
        if i == -1:
            for w in sb:
                w.near()
            heard_above(0)
            pass_down(0)
    for w in sb:
        w.far()
    for i in (0, -1, 1, 2):
        for w in sb:
            w.turn(i)
        for w in sa:
            w.end(i)
    a_mates, mates = mates, []

    for k in (-1, 5, 1):
        spread(k).wait_recv()
    line = pb.at[c, y]
    py = [net.send(line, line, d) for d in (yo, yp, ym)]

    lx.wait()
    for copy in small:
        copy.wait()

    def norm_cand(cc):
        rows = pl.ds(128 * cc, 128)
        into = pl.ds(NPRE + 128 * cc, 128)
        total = jnp.zeros((128, 1), F32)
        for f in range(4):
            v = xb[f, rows, :].astype(F32)
            total += jnp.sum(v * v, axis=-1, keepdims=True)
        scale = lax.rsqrt(total * (1.0 / D) + EPS)
        for f in range(4):
            v = xb[f, rows, :].astype(F32)
            g = gain[:, FC * f : FC * (f + 1)]
            xn[into, FC * f : FC * (f + 1)] = (v * scale * g).astype(BF16)

    for copy in st[0]:
        copy.wait_recv()
    norm_cand(0)

    for copy in a_mates:
        copy.wait_recv()

    def rotate(v, cos, sin):
        a, b = v[:, :128], v[:, 128:]
        return jnp.concatenate([a * cos - b * sin, b * cos + a * sin], axis=-1)

    def project_q(cc):
        xrows = pl.ds(NPRE + 128 * cc, 128)

        def head(r, carry):
            qv = jnp.dot(xn[xrows, :], A[r], preferred_element_type=F32)
            qv = rotate(qv, cos_t[PRE:, :], sin_t[PRE:, :]) * (HS ** -0.5)
            q4[cc, pl.ds(pl.multiple_of(r * CL, CL), CL), :] = qv.astype(BF16)
            return carry

        lax.fori_loop(0, 4, head, 0)

    for copy in py:
        copy.wait_recv()
    pm = net.send(pb.at[c], pb.at[c], mate)
    project_q(0)

    for i in (0, -1):
        for w in sb:
            w.end(i)

    pm.wait_recv()
    for f in range(4):
        for g in range(32):
            pf[f, 2 * g : 2 * g + 2, :] = pb[g // 16, (g // 4) % 4, (g % 4) * 4 + f].astype(F32)
    total = jnp.zeros((PRE, 1), F32)
    for f in range(4):
        total += jnp.sum(pf[f] * pf[f], axis=-1, keepdims=True)
    scale = lax.rsqrt(total * (1.0 / D) + EPS)
    for f in range(4):
        g = gain[:, FC * f : FC * (f + 1)]
        xn[0:PRE, FC * f : FC * (f + 1)] = (pf[f] * scale * g).astype(BF16)

    for copy in st[1]:
        copy.wait_recv()
    norm_cand(1)
    project_q(1)

    for i in (1, 2):
        for w in sb:
            w.end(i)
    for copy in mates:
        copy.wait_recv()

    for pair in range(2):
        w = jnp.concatenate([B[2 * pair, 256:384, :], B[2 * pair + 1, 256:384, :]], axis=0)
        r = lax.dot_general(xn[...], w, (((1,), (1,)), ((), ())), preferred_element_type=F32)
        kvs[2 * pair] = r[:, :128]
        kvs[2 * pair + 1] = r[:, 128:]
    parts = [kvs[(f - t + 4) % 4] for f in range(4)]
    key = jnp.concatenate([p[:, :64] for p in parts], axis=-1)
    vc[...] = jnp.concatenate([p[:, 64:] for p in parts], axis=-1).astype(BF16)
    kc[0 : PRE + CL, :] = rotate(key[: PRE + CL], cos_t[...], sin_t[...]).astype(BF16)
    kc[PRE + CL :, :] = rotate(key[PRE + CL :], cos_t[PRE:, :], sin_t[PRE:, :]).astype(BF16)

    for cc in range(2):
        own = PRE + CL * cc
        keys = jnp.concatenate([kc[0:PRE, :], kc[own : own + CL, :]], axis=0)
        vals = jnp.concatenate([vc[0:PRE, :], vc[own : own + CL, :]], axis=0)
        live = lens[2 * t + cc]
        scores = lax.dot_general(
            q4[cc], keys, (((1,), (1,)), ((), ())), preferred_element_type=F32
        )
        row = lax.broadcasted_iota(jnp.int32, scores.shape, 0) % CL
        col = lax.broadcasted_iota(jnp.int32, scores.shape, 1)
        scores = jnp.where(col <= row + PRE, scores, -jnp.inf)
        weights = jnp.exp(scores - jnp.max(scores, axis=-1, keepdims=True))
        divisor = jnp.sum(weights, axis=-1, keepdims=True)
        mix = jnp.dot(weights.astype(BF16), vals, preferred_element_type=F32) / divisor
        slot = lax.broadcasted_iota(jnp.int32, mix.shape, 0) % CL
        mix = jnp.where(slot < live, mix, 0.0).astype(BF16)
        for r in range(4):
            hr[CL * cc : CL * (cc + 1), HS * r : HS * (r + 1)] = mix[r * CL : (r + 1) * CL]

    def out_cols(n, carry):
        cols = pl.ds(pl.multiple_of(n * 512, 512), 512)
        acc = jnp.zeros((256, 512), F32)
        for r in range(4):
            acc += jnp.dot(
                hr[:, HS * r : HS * (r + 1)], B[r, 0:256, cols], preferred_element_type=F32
            )
        ob[:, cols] = acc.astype(BF16)
        pltpu.make_async_copy(ob.at[:, cols], out.at[:, cols], lsem.at[11 + n]).start()
        return carry

    lax.fori_loop(0, 4, out_cols, 0)
    outs = []
    for n in range(4):
        cols = pl.ds(n * 512, 512)
        outs.append(pltpu.make_async_copy(ob.at[:, cols], out.at[:, cols], lsem.at[11 + n]))

    net.finish()
    for end, ks in ways:
        @pl.when(t == end)
        def _(ks=ks):
            for k in ks:
                spread(k).wait_send()

    for copy in outs:
        copy.wait()


def body(cand_states, prefix_states, norm_gain, w_query, w_key, w_value, w_out, cand_lengths):
    cos_np, sin_np = rope_tables()
    any_spec = pl.BlockSpec(memory_space=pl.ANY)
    return pl.pallas_call(
        kernel,
        out_shape=jax.ShapeDtypeStruct((256, D), BF16),
        in_specs=[any_spec] * 10,
        out_specs=any_spec,
        scratch_shapes=[
            pltpu.VMEM((4, D, HS), BF16),
            pltpu.VMEM((4, 384, D), BF16),
            pltpu.VMEM((1024, FC), BF16),
            pltpu.VMEM((4, 256, FC), BF16),
            pltpu.VMEM((2, 4, 16, 2, FC), BF16),
            pltpu.VMEM((4, PRE, FC), F32),
            pltpu.VMEM((320, D), BF16),
            pltpu.VMEM((4, 320, 128), F32),
            pltpu.VMEM((320, HS), BF16),
            pltpu.VMEM((320, HS), BF16),
            pltpu.VMEM((2, 4 * CL, HS), BF16),
            pltpu.VMEM((256, 4 * HS), BF16),
            pltpu.VMEM((256, D), BF16),
            pltpu.VMEM((1, D), F32),
            pltpu.VMEM((PRE + CL, 128), F32),
            pltpu.VMEM((PRE + CL, 128), F32),
            pltpu.SMEM((8,), jnp.int32),
            pltpu.SemaphoreType.DMA((N_SEMS,)),
            pltpu.SemaphoreType.DMA((N_SEMS,)),
            pltpu.SemaphoreType.DMA((16,)),
            pltpu.SemaphoreType.DMA((12,)),
            pltpu.SemaphoreType.DMA((3,)),
            pltpu.SemaphoreType.REGULAR,
            pltpu.SemaphoreType.REGULAR,
            pltpu.SemaphoreType.REGULAR,
            pltpu.SemaphoreType.REGULAR,
        ],
        compiler_params=pltpu.CompilerParams(
            collective_id=0, has_side_effects=True, vmem_limit_bytes=56 * 1024 * 1024
        ),
        name="sublayer",
    )(
        cand_states, prefix_states, norm_gain.reshape(1, D), w_query, w_key.T, w_value.T,
        w_out, cand_lengths, jnp.asarray(cos_np), jnp.asarray(sin_np),
    )


def solution(mesh):
    in_specs = (
        P(("query", "cand"), "tensor"),
        P(("query", "cand"), "tensor"),
        P(),
        P(None, "tensor"),
        P(None, "tensor"),
        P(None, "tensor"),
        P("tensor", None),
        P(("query", "cand")),
    )
    out_specs = P(("query", "cand", "tensor"), None)
    return jax.shard_map(body, mesh=mesh, in_specs=in_specs, out_specs=out_specs, check_vma=False)
```

```python
import numpy as np

import jax
import jax.numpy as jnp
from jax import lax
from jax.experimental import pallas as pl
from jax.experimental.pallas import tpu as pltpu
from jax.sharding import PartitionSpec as P

MESH = pl.DeviceIdType.MESH
BF16 = jnp.bfloat16
F32 = jnp.float32
EPS = 1e-06
THETA = 10000.0

NX = 4
NY = 4
NZ = 16
ZL = 4
CL = 128
HS = 256
D = 2048
FC = 512
PRE = 64


def rope_tables():
    half = HS // 2
    freq = (THETA ** (-np.arange(half, dtype=np.float32) * 2.0 / HS)).astype(np.float32)
    cand = (PRE + np.arange(CL)).astype(np.float32)
    core, y, zh, r = np.meshgrid(
        np.arange(2), np.arange(4), np.arange(4), np.arange(2), indexing="ij"
    )
    pre = ((zh * 8 + y * 2 + core) * 2 + r).reshape(-1).astype(np.float32)
    pos = np.concatenate([pre, cand])
    angles = (pos[:, None] * freq[None, :]).astype(np.float32).astype(np.float64)
    return np.cos(angles).astype(np.float32), np.sin(angles).astype(np.float32)


class Links:
    def __init__(self, ssem, rsem):
        self.ssem, self.rsem, self.made = ssem, rsem, []

    def send(self, src, dst, device):
        i = len(self.made)
        copy = pltpu.make_async_remote_copy(
            src_ref=src,
            dst_ref=dst,
            send_sem=self.ssem.at[i],
            recv_sem=self.rsem.at[i],
            device_id=device,
            device_id_type=MESH,
        )
        copy.start()
        self.made.append(copy)
        return copy

    def finish(self):
        for copy in self.made:
            copy.wait_send()


N_SEMS = 136
NPRE = PRE


def kernel(
    states, prefix, gain_h, wq, wk, wv, wo, lens_h, cos_h, sin_h,
    out,
    A, B, xs, xb, pb, pf, xn, kvs, kc, vc, q4, hr, ob, gain, cos_t, sin_t, lens,
    ssem, rsem, lsem, psem, qsem, go, chain, go_dn, chain_dn,
):
    x = lax.axis_index("query")
    cd = lax.axis_index("cand")
    t = lax.axis_index("tensor")
    zh = cd // 8
    y = (cd // 2) % 4
    c = cd % 2
    z = zh * 4 + t

    def at(xx, yy, zz, cc):
        return (xx, (zz // 4) * 8 + yy * 2 + cc, zz % 4)

    def m4(v):
        return (v + 8) % 4

    def zdev(dz):
        return at(x, y, (z + dz + 32) % 16, c)

    def tdev(k):
        return (x, cd, (t + k) % 4)

    xp, xm = at(m4(x + 1), y, z, c), at(m4(x - 1), y, z, c)
    yp, ym = at(x, m4(y + 1), z, c), at(x, m4(y - 1), z, c)
    yo = at(x, m4(y + 2), z, c)
    mate = at(x, y, z, 1 - c)

    def part_a(s, first, second, off=0, n=32, q=slice(1, 4)):
        row = c * 1024 + s * 512 + 32 * (second * 4 + first) + off
        return A.at[q, pl.ds(pl.multiple_of(row, 16), n), :]

    def part_b(s, first, second, off=0, n=96, q=slice(1, 4)):
        row = 192 * c + 96 * s + off
        col = 128 * (second * 4 + first)
        return B.at[
            q, pl.ds(pl.multiple_of(row, 16), n), pl.ds(pl.multiple_of(col, 128), 128)
        ]

    def set_a(s, second):
        row = c * 1024 + s * 512 + 128 * second
        return A.at[1:4, pl.ds(pl.multiple_of(row, 128), 128), :]

    def set_b(s, second):
        row, col = 192 * c + 96 * s, 512 * second
        return B.at[
            1:4, pl.ds(pl.multiple_of(row, 32), 96), pl.ds(pl.multiple_of(col, 512), 512)
        ]

    def local(i, src, dst):
        copy = pltpu.make_async_copy(src, dst, lsem.at[i])
        copy.start()
        return copy

    lp = local(0, prefix, pb.at[c, y, z])
    lq = local(1, wq, A.at[0])
    lo = [
        local(2, wk, B.at[0, 256:320, :]),
        local(3, wv, B.at[0, 320:384, :]),
        local(4, wo, B.at[0, 0:256, :]),
    ]
    ls = local(5, states, xs)
    lx = local(6, states.at[pl.ds(pl.multiple_of(256 * t, 256), 256), :], xb.at[t])
    small = [
        local(7, gain_h, gain),
        local(8, cos_h, cos_t),
        local(9, sin_h, sin_t),
        local(10, lens_h, lens),
    ]

    up_edge = (t == 3) & (zh < 3)
    down_edge = (t == 0) & (zh > 0)
    up1, down1 = zdev(1), zdev(-1)
    barrier = pltpu.get_barrier_semaphore()
    near = [tdev(1), tdev(2), tdev(3), xp, xm, yp, ym, yo, mate]
    for device in near:
        pl.semaphore_signal(barrier, inc=1, device_id=device, device_id_type=MESH)

    @pl.when(up_edge)
    def _():
        pl.semaphore_signal(barrier, inc=1, device_id=up1, device_id_type=MESH)

    @pl.when(down_edge)
    def _():
        pl.semaphore_signal(barrier, inc=1, device_id=down1, device_id_type=MESH)

    edge = up_edge.astype(jnp.int32) + down_edge.astype(jnp.int32)
    pl.semaphore_wait(barrier, len(near) + edge)

    @pl.when(down_edge)
    def _():
        @pl.when(zh == 3)
        def _():
            pl.semaphore_signal(go_dn, inc=1, device_id=down1, device_id_type=MESH)

        pl.semaphore_wait(go, 1)
        pl.semaphore_signal(chain, inc=1, device_id=tdev(3), device_id_type=MESH)

    @pl.when(up_edge)
    def _():
        @pl.when(zh > 0)
        def _():
            pl.semaphore_wait(chain, 1)

        pl.semaphore_signal(go, inc=1, device_id=up1, device_id_type=MESH)

    @pl.when((t == 3) & (zh == 3))
    def _():
        pl.semaphore_wait(chain, 1)

    net = Links(ssem, rsem)

    lp.wait()
    tile = pb.at[c, y, z]
    pz = [net.send(tile, tile, tdev(k)) for k in (2, 1, 3)]

    def block_set(b):
        b = (b + 4) % 4
        return pb.at[c, y, pl.ds(pl.multiple_of(4 * b, 4), 4)]

    def spread(k):
        moved = block_set(zh)
        far = 1 if abs(k) > 4 else (2 if k > 0 else 0)
        return pltpu.make_async_remote_copy(
            src_ref=moved,
            dst_ref=moved,
            send_sem=psem.at[k - 1 if k > 0 else 5 - k],
            recv_sem=qsem.at[far],
            device_id=zdev(k),
            device_id_type=MESH,
        )

    ways = ((3, (6, 5, 4, 3, 2, 1)), (0, (-6, -5, -4, -3, -2, -1)))

    def spread_from(end):
        for k in ways[0][1] if end == 3 else ways[1][1]:
            spread(k).start()

    def heard_above(b):
        @pl.when((t == 3) & (zh == b))
        def _():
            pl.semaphore_wait(go_dn, 1)
            pl.semaphore_signal(chain_dn, inc=1, device_id=tdev(1), device_id_type=MESH)
            spread_from(3)

    def pass_down(b):
        @pl.when((t == 0) & (zh == b))
        def _():
            pl.semaphore_wait(chain_dn, 1)
            if b > 0:
                pl.semaphore_signal(go_dn, inc=1, device_id=down1, device_id_type=MESH)
            if b < 2:
                spread_from(0)

    def slices(part, q=slice(1, 4)):
        return part(0, x, y, q=q), part(1, y, x, q=q)

    def to_peers(part):
        sent = []
        for k in (2, 1, 3):
            for src, dst in zip(slices(part, 0), slices(part, 4 - k)):
                sent.append(net.send(src, dst, tdev(k)))
        return sent

    lq.wait()
    pa = to_peers(part_a)
    for copy in lo:
        copy.wait()
    pbq = to_peers(part_b)

    ls.wait()
    st = []
    for cc in range(2):
        part = []
        for k in (2, 1, 3):
            peer = (t + k) % 4
            src = xs.at[pl.ds(pl.multiple_of(256 * peer + 128 * cc, 128), 128), :]
            dst = xb.at[t, pl.ds(128 * cc, 128), :]
            part.append(net.send(src, dst, tdev(k)))
        st.append(part)

    mates = []

    class Stream:
        def __init__(self, part, whole, s, n):
            self.part = lambda i, j, off=0, n=n: part(s, m4(self.me[0] + i), m4(self.me[1] + j), off, n)
            self.whole = lambda j: whole(s, m4(self.me[1] + j))
            self.me = (x, y) if s == 0 else (y, x)
            self.first = (xp, xm) if s == 0 else (yp, ym)
            self.second = (yp, ym) if s == 0 else (xp, xm)
            self.half = n // 2
            self.onward = {}

        def both(self, piece, dirs):
            return tuple(net.send(piece, piece, d) for d in dirs)

        def own(self):
            piece = self.part(0, 0)
            self.near_copies = self.both(piece, self.first)
            self.onward[0] = self.both(piece, self.second)

        def near(self):
            self.far_copies = []
            for side, i in ((0, -1), (1, 1)):
                self.near_copies[side].wait_recv()
                h = self.part(i, 0, side * self.half, self.half)
                self.far_copies.append(net.send(h, h, self.first[side]))
                self.onward[i] = self.both(self.part(i, 0), self.second)

        def far(self):
            for copy in self.far_copies:
                copy.wait_recv()
            self.onward[2] = self.both(self.part(2, 0), self.second)
            mates.append(net.send(self.whole(0), self.whole(0), mate))

        def turn(self, i):
            self.last = getattr(self, "last", {})
            self.last[i] = []
            for side, j in ((0, -1), (1, 1)):
                self.onward[i][side].wait_recv()
                h = self.part(i, j, side * self.half, self.half)
                self.last[i].append(net.send(h, h, self.second[side]))
            if i == 2:
                for j in (-1, 1):
                    mates.append(net.send(self.whole(j), self.whole(j), mate))

        def end(self, i):
            for copy in self.last[i]:
                copy.wait_recv()
            s = self.part(i, 2)
            mates.append(net.send(s, s, mate))

    sa = [Stream(part_a, set_a, s, 32) for s in (0, 1)]
    sb = [Stream(part_b, set_b, s, 96) for s in (0, 1)]
    for copy in pa:
        copy.wait_recv()
    for w in sa:
        w.own()
    for copy in pz:
        copy.wait_recv()
    @pl.when((t == 3) & (zh == 3))
    def _():
        spread_from(3)

    @pl.when((t == 0) & (zh >= 2))
    def _():
        spread_from(0)

    heard_above(2)
    for w in sa:
        w.near()
    pass_down(2)
    for copy in pbq:
        copy.wait_recv()
    for w in sb:
        w.own()
    for w in sa:
        w.far()
    heard_above(1)
    pass_down(1)
    for i in (0, -1, 1, 2):
        for w in sa:
            w.turn(i)
        if i == -1:
            for w in sb:
                w.near()
            heard_above(0)
            pass_down(0)
    for w in sb:
        w.far()
    for i in (0, -1, 1, 2):
        for w in sb:
            w.turn(i)
        for w in sa:
            w.end(i)
    a_mates, mates = mates, []

    for k in (-1, 5, 1):
        spread(k).wait_recv()
    line = pb.at[c, y]
    py = [net.send(line, line, d) for d in (yo, yp, ym)]

    lx.wait()
    for copy in small:
        copy.wait()

    def norm_cand(cc):
        rows = pl.ds(128 * cc, 128)
        into = pl.ds(NPRE + 128 * cc, 128)
        total = jnp.zeros((128, 1), F32)
        for f in range(4):
            v = xb[f, rows, :].astype(F32)
            total += jnp.sum(v * v, axis=-1, keepdims=True)
        scale = lax.rsqrt(total * (1.0 / D) + EPS)
        for f in range(4):
            v = xb[f, rows, :].astype(F32)
            g = gain[:, FC * f : FC * (f + 1)]
            xn[into, FC * f : FC * (f + 1)] = (v * scale * g).astype(BF16)

    for copy in st[0]:
        copy.wait_recv()
    norm_cand(0)

    for copy in a_mates:
        copy.wait_recv()

    def rotate(v, cos, sin):
        a, b = v[:, :128], v[:, 128:]
        return jnp.concatenate([a * cos - b * sin, b * cos + a * sin], axis=-1)

    def project_q(cc):
        xrows = pl.ds(NPRE + 128 * cc, 128)

        def head(r, carry):
            qv = jnp.dot(xn[xrows, :], A[r], preferred_element_type=F32)
            qv = rotate(qv, cos_t[PRE:, :], sin_t[PRE:, :]) * (HS ** -0.5)
            q4[cc, pl.ds(pl.multiple_of(r * CL, CL), CL), :] = qv.astype(BF16)
            return carry

        lax.fori_loop(0, 4, head, 0)

    for copy in py:
        copy.wait_recv()
    pm = net.send(pb.at[c], pb.at[c], mate)
    project_q(0)

    for i in (0, -1):
        for w in sb:
            w.end(i)

    pm.wait_recv()
    for f in range(4):
        for g in range(32):
            pf[f, 2 * g : 2 * g + 2, :] = pb[g // 16, (g // 4) % 4, (g % 4) * 4 + f].astype(F32)
    total = jnp.zeros((PRE, 1), F32)
    for f in range(4):
        total += jnp.sum(pf[f] * pf[f], axis=-1, keepdims=True)
    scale = lax.rsqrt(total * (1.0 / D) + EPS)
    for f in range(4):
        g = gain[:, FC * f : FC * (f + 1)]
        xn[0:PRE, FC * f : FC * (f + 1)] = (pf[f] * scale * g).astype(BF16)

    for i in (1, 2):
        for w in sb:
            w.end(i)

    for copy in st[1]:
        copy.wait_recv()
    norm_cand(1)
    project_q(1)

    for copy in mates:
        copy.wait_recv()

    for pair in range(2):
        w = jnp.concatenate([B[2 * pair, 256:384, :], B[2 * pair + 1, 256:384, :]], axis=0)
        r = lax.dot_general(xn[...], w, (((1,), (1,)), ((), ())), preferred_element_type=F32)
        kvs[2 * pair] = r[:, :128]
        kvs[2 * pair + 1] = r[:, 128:]
    parts = [kvs[(f - t + 4) % 4] for f in range(4)]
    key = jnp.concatenate([p[:, :64] for p in parts], axis=-1)
    vc[...] = jnp.concatenate([p[:, 64:] for p in parts], axis=-1).astype(BF16)
    kc[0 : PRE + CL, :] = rotate(key[: PRE + CL], cos_t[...], sin_t[...]).astype(BF16)
    kc[PRE + CL :, :] = rotate(key[PRE + CL :], cos_t[PRE:, :], sin_t[PRE:, :]).astype(BF16)

    for cc in range(2):
        own = PRE + CL * cc
        keys = jnp.concatenate([kc[0:PRE, :], kc[own : own + CL, :]], axis=0)
        vals = jnp.concatenate([vc[0:PRE, :], vc[own : own + CL, :]], axis=0)
        live = lens[2 * t + cc]
        scores = lax.dot_general(
            q4[cc], keys, (((1,), (1,)), ((), ())), preferred_element_type=F32
        )
        row = lax.broadcasted_iota(jnp.int32, scores.shape, 0) % CL
        col = lax.broadcasted_iota(jnp.int32, scores.shape, 1)
        scores = jnp.where(col <= row + PRE, scores, -jnp.inf)
        weights = jnp.exp(scores - jnp.max(scores, axis=-1, keepdims=True))
        divisor = jnp.sum(weights, axis=-1, keepdims=True)
        mix = jnp.dot(weights.astype(BF16), vals, preferred_element_type=F32) / divisor
        slot = lax.broadcasted_iota(jnp.int32, mix.shape, 0) % CL
        mix = jnp.where(slot < live, mix, 0.0).astype(BF16)
        for r in range(4):
            hr[CL * cc : CL * (cc + 1), HS * r : HS * (r + 1)] = mix[r * CL : (r + 1) * CL]

    def out_cols(n, carry):
        cols = pl.ds(pl.multiple_of(n * 512, 512), 512)
        acc = jnp.zeros((256, 512), F32)
        for r in range(4):
            acc += jnp.dot(
                hr[:, HS * r : HS * (r + 1)], B[r, 0:256, cols], preferred_element_type=F32
            )
        ob[:, cols] = acc.astype(BF16)
        pltpu.make_async_copy(ob.at[:, cols], out.at[:, cols], lsem.at[11 + n]).start()
        return carry

    lax.fori_loop(0, 4, out_cols, 0)
    outs = []
    for n in range(4):
        cols = pl.ds(n * 512, 512)
        outs.append(pltpu.make_async_copy(ob.at[:, cols], out.at[:, cols], lsem.at[11 + n]))

    net.finish()
    for end, ks in ways:
        @pl.when(t == end)
        def _(ks=ks):
            for k in ks:
                spread(k).wait_send()

    for copy in outs:
        copy.wait()


def body(cand_states, prefix_states, norm_gain, w_query, w_key, w_value, w_out, cand_lengths):
    cos_np, sin_np = rope_tables()
    any_spec = pl.BlockSpec(memory_space=pl.ANY)
    return pl.pallas_call(
        kernel,
        out_shape=jax.ShapeDtypeStruct((256, D), BF16),
        in_specs=[any_spec] * 10,
        out_specs=any_spec,
        scratch_shapes=[
            pltpu.VMEM((4, D, HS), BF16),
            pltpu.VMEM((4, 384, D), BF16),
            pltpu.VMEM((1024, FC), BF16),
            pltpu.VMEM((4, 256, FC), BF16),
            pltpu.VMEM((2, 4, 16, 2, FC), BF16),
            pltpu.VMEM((4, PRE, FC), F32),
            pltpu.VMEM((320, D), BF16),
            pltpu.VMEM((4, 320, 128), F32),
            pltpu.VMEM((320, HS), BF16),
            pltpu.VMEM((320, HS), BF16),
            pltpu.VMEM((2, 4 * CL, HS), BF16),
            pltpu.VMEM((256, 4 * HS), BF16),
            pltpu.VMEM((256, D), BF16),
            pltpu.VMEM((1, D), F32),
            pltpu.VMEM((PRE + CL, 128), F32),
            pltpu.VMEM((PRE + CL, 128), F32),
            pltpu.SMEM((8,), jnp.int32),
            pltpu.SemaphoreType.DMA((N_SEMS,)),
            pltpu.SemaphoreType.DMA((N_SEMS,)),
            pltpu.SemaphoreType.DMA((16,)),
            pltpu.SemaphoreType.DMA((12,)),
            pltpu.SemaphoreType.DMA((3,)),
            pltpu.SemaphoreType.REGULAR,
            pltpu.SemaphoreType.REGULAR,
            pltpu.SemaphoreType.REGULAR,
            pltpu.SemaphoreType.REGULAR,
        ],
        compiler_params=pltpu.CompilerParams(
            collective_id=0, has_side_effects=True, vmem_limit_bytes=56 * 1024 * 1024
        ),
        name="sublayer",
    )(
        cand_states, prefix_states, norm_gain.reshape(1, D), w_query, w_key.T, w_value.T,
        w_out, cand_lengths, jnp.asarray(cos_np), jnp.asarray(sin_np),
    )


def solution(mesh):
    in_specs = (
        P(("query", "cand"), "tensor"),
        P(("query", "cand"), "tensor"),
        P(),
        P(None, "tensor"),
        P(None, "tensor"),
        P(None, "tensor"),
        P("tensor", None),
        P(("query", "cand")),
    )
    out_specs = P(("query", "cand", "tensor"), None)
    return jax.shard_map(body, mesh=mesh, in_specs=in_specs, out_specs=out_specs, check_vma=False)
```
